128 devices in a mesh: section: 8 (over y, core), dp: 16 (over z, x).
Axes of the slice: x: 4, y: 4, z: 4, core: 2. Of those that a mesh axis runs over, the one named last changes fastest.
Arguments:
- acts: bfloat16 [8, 8192, 3584], P('section', 'dp'), may hold values from -400 to 400
- cotangent: bfloat16 [8192, 3584], P('dp'), may hold values from -6 to 6
- frozen: bfloat16 [8, 3584, 3584], P('section', 'dp'), may hold values from -0.09375 to 0.09375
- down_adapter: bfloat16 [8, 16, 3584], P('section'), may hold values from -0.25 to 0.25
- up_adapter: bfloat16 [8, 16, 3584], P('section'), may hold values from -0.25 to 0.25
- example_ids: int32 [16, 4], P('dp'), may hold values from 0 to 3, each once within a row
- lengths: int32 [16, 4], P('dp'), may hold values from 32 to 128
Outputs:
- grad_down: float32 [8, 16, 3584], P('section', None, 'dp')
- grad_up: float32 [8, 16, 3584], P('section', None, 'dp')
- example_norms: float32 [16, 4], P('dp')
The draws below stay inside these ranges and needn't reach their ends.
Inputs may be any that keep to these rules, and one draw needn't show every extreme that they name: `example_ids`: each row is an ordering of the 4 examples of one replica.
All inputs are finite; a program needn't handle non-finite values.
Results may differ from the reference program's by a relative error of at most 0.009.
Values may be sent and summed in bfloat16 or wider, within the bound.
A program may use at most 128 MiB of HBM per device.

```python
import math
import jax
import jax.numpy as jnp
from jax import lax

DW = 3584
RANK = 16
MICRO = 4
SEQ = 128
SECTIONS = 8
REPLICAS = 16
EXAMPLES = 64
TOKENS = 8192


def draw_acts(key, part):
    keys = jax.random.split(jax.random.fold_in(key, 17), 4)
    section_pos = jnp.arange(SECTIONS, dtype=jnp.float32) / max(SECTIONS - 1, 1)
    base = jax.random.truncated_normal(keys[0], -4.0, 4.0, (SECTIONS, TOKENS, DW), jnp.float32)
    section_scale = 3.0 ** section_pos
    row_scale = jnp.exp(jax.random.uniform(keys[2], (SECTIONS, TOKENS, 1), jnp.float32, -1.15, 1.15))
    col_scale = jnp.exp(jax.random.uniform(keys[3], (SECTIONS, 1, DW), jnp.float32, -1.15, 1.15))
    return (base * row_scale * col_scale * section_scale[:, None, None]).astype(jnp.bfloat16)


def touch_ends(values, stream_key, smallest, high):
    longest = values.shape.index(max(values.shape))
    spots = []
    for shift in (0, 1):
        where = [jax.random.randint(jax.random.fold_in(stream_key, axis), (), 0, length) for axis, length in enumerate(values.shape)]
        where[longest] = (where[longest] + shift) % values.shape[longest]
        spots.append(tuple(where))
    return values.at[spots[0]].set(smallest).at[spots[1]].set(high)


def block_scale(own_key, dims, pieces, least, top_value):
    def one(dim, blocks):
        heights = jax.random.uniform(jax.random.fold_in(jax.random.fold_in(own_key, 6), dim), (blocks,), jnp.float32, least / len(pieces), top_value / len(pieces))
        return jnp.repeat(jnp.exp(heights), dims[dim] // blocks).reshape((-1,) + (1,) * (len(dims) - dim - 1))

    factor_of = one(*pieces[0])
    for cut in pieces[1:]:
        factor_of = factor_of * one(*cut)
    return factor_of


def scatter_about(own_key, dims, deviation, most, shards=(), kind=jnp.bfloat16):
    array = deviation * jax.random.normal(own_key, dims, jnp.float32)
    if shards:
        array = array * block_scale(own_key, dims, shards, -0.22, 0.18)
    return jnp.clip(array, -most, most).astype(kind)


def setup_inputs(seed: int = 0) -> dict:
    seeds = jax.random.split(jax.random.key(seed), 8)
    acts = draw_acts(jax.random.fold_in(seeds[7], 71), 0)
    cotangent = scatter_about(seeds[1], (TOKENS, DW), 1.0, 6.0, ((0, 16),))
    frozen = scatter_about(seeds[2], (SECTIONS, DW, DW), (DW * 5 // 4) ** -0.5, 0.09375, ((0, 8), (1, 16)))
    down_adapter = scatter_about(seeds[3], (SECTIONS, RANK, DW), ((5 * RANK * DW) ** 0.5) ** -0.5, 0.25, ((0, 8),))
    up_adapter = scatter_about(seeds[4], (SECTIONS, RANK, DW), ((5 * RANK * DW) ** 0.5) ** -0.5, 0.25, ((0, 8),))
    example_ids = jax.vmap(lambda own: jax.random.permutation(own, MICRO))(jax.random.split(seeds[5], REPLICAS)).reshape((REPLICAS, MICRO)).astype(jnp.int32)
    lengths = touch_ends(jax.random.randint(seeds[6], (REPLICAS, MICRO), SEQ // 4, SEQ + 1), jax.random.fold_in(seeds[6], 1), SEQ // 4, SEQ).astype(jnp.int32)
    return {"acts": acts, "cotangent": cotangent, "frozen": frozen, "down_adapter": down_adapter, "up_adapter": up_adapter, "example_ids": example_ids, "lengths": lengths}


def reference(acts, cotangent, frozen, down_adapter, up_adapter, example_ids, lengths):
    choose = (example_ids[:, :, None] == jnp.arange(MICRO, dtype=jnp.int32)[None, None, :]).astype(jnp.int32)
    slot_length = lax.optimization_barrier(jnp.sum(choose * lengths[:, None, :], axis=2))
    live = (jnp.arange(SEQ, dtype=jnp.int32)[None, None, :] < slot_length[:, :, None]).astype(jnp.bfloat16)
    out_grad = cotangent * live.reshape(TOKENS, 1)
    down_terms = []
    up_terms = []
    square_sum = jnp.zeros((EXAMPLES,), jnp.float32)
    for section in range(SECTIONS - 1, -1, -1):
        inputs = acts[section]
        up_grad = jnp.dot(out_grad, up_adapter[section].T, preferred_element_type=jnp.float32).astype(jnp.bfloat16)
        down_act = jnp.dot(inputs, down_adapter[section].T, preferred_element_type=jnp.float32).astype(jnp.bfloat16)
        down_term = jnp.einsum('esr,esd->erd', up_grad.reshape(EXAMPLES, SEQ, RANK).astype(jnp.float32), inputs.reshape(EXAMPLES, SEQ, DW).astype(jnp.float32))
        up_term = jnp.einsum('esr,esd->erd', down_act.reshape(EXAMPLES, SEQ, RANK).astype(jnp.float32), out_grad.reshape(EXAMPLES, SEQ, DW).astype(jnp.float32))
        square_sum = square_sum + lax.optimization_barrier(jnp.sum(down_term * down_term, axis=(1, 2))) + lax.optimization_barrier(jnp.sum(up_term * up_term, axis=(1, 2)))
        down_terms.append(down_term)
        up_terms.append(up_term)
        in_grad = jnp.dot(out_grad, frozen[section].T, preferred_element_type=jnp.float32)
        in_grad = in_grad + jnp.dot(up_grad, down_adapter[section], preferred_element_type=jnp.float32)
        out_grad = in_grad.astype(jnp.bfloat16)
    norm = jnp.sqrt(square_sum)
    factor = math.sqrt(2.0 * RANK * DW) / ((norm + 0.01) * math.sqrt(EXAMPLES))
    down_terms = down_terms[::-1]
    up_terms = up_terms[::-1]
    grad_down = jnp.stack([lax.optimization_barrier(jnp.sum(factor[:, None, None] * term, axis=0)) for term in down_terms])
    grad_up = jnp.stack([lax.optimization_barrier(jnp.sum(factor[:, None, None] * term, axis=0)) for term in up_terms])
    slot_norm = norm.reshape(REPLICAS, MICRO)
    example_norms = lax.optimization_barrier(jnp.sum(choose.astype(jnp.float32) * slot_norm[:, :, None], axis=1))
    return (grad_down, grad_up, example_norms)
```

```python
import functools
import math

import jax
import jax.numpy as jnp
from jax import lax
from jax.experimental import pallas as pl
from jax.experimental.pallas import tpu as pltpu
from jax.sharding import PartitionSpec as P

MESH = pl.DeviceIdType.MESH
NT = (((1,), (1,)), ((), ()))
CHUNKS = 7
LANES = 128


def fdot(a, b, dims=None):
    if dims is None:
        return jnp.dot(a, b, preferred_element_type=jnp.float32)
    return lax.dot_general(a, b, dims, preferred_element_type=jnp.float32)


def kernel(
    sections, replicas, clip_scale,
    w_hbm, seed_hbm, acts_hbm, up_ref, down_ref, downt_ref,
    red_ref, norm_ref,
    wbuf, gbuf, obuf, abuf, ugbuf, dabuf, tbuf, sqbuf, sqall, redsend, redin,
    w_sem, seed_sem, a_sem, send_sem, recv_sem, sqs_sem, sqr_sem, rs_sem, rr_sem,
):
    s = lax.axis_index("section")
    d = lax.axis_index("dp")
    slots, features, tokens = gbuf.shape
    rank = up_ref.shape[0]
    rows = features // CHUNKS
    span = features // replicas
    window = redin.shape[2]

    barrier = pltpu.get_barrier_semaphore()
    for k in range(1, sections):
        pl.semaphore_signal(barrier, inc=1, device_id=((s + k) % sections, d), device_id_type=MESH)
    for k in range(1, replicas):
        pl.semaphore_signal(barrier, inc=1, device_id=(s, (d + k) % replicas), device_id_type=MESH)

    def w_copy(c):
        at = pl.ds(c * rows, rows)
        return pltpu.make_async_copy(w_hbm.at[at], wbuf.at[at], w_sem.at[c])

    seed_copy = pltpu.make_async_copy(seed_hbm, gbuf, seed_sem)
    acts_copy = pltpu.make_async_copy(acts_hbm, abuf, a_sem)

    @pl.when(s == sections - 1)
    def _():
        seed_copy.start()

    acts_copy.start()

    @pl.when(s > 0)
    def _():
        for c in range(CHUNKS):
            w_copy(c).start()

    acts_copy.wait()
    dabuf[...] = fdot(down_ref[...], abuf[...], NT).astype(jnp.bfloat16)

    @pl.when(s == sections - 1)
    def _():
        seed_copy.wait()

    @pl.when(s > 0)
    def _():
        for c in range(CHUNKS):
            w_copy(c).wait()

    pl.semaphore_wait(barrier, sections - 1 + replicas - 1)

    def hop(m, c):
        at = pl.ds(pl.multiple_of(c * rows, rows), rows)
        return pltpu.make_async_remote_copy(
            src_ref=obuf.at[m, at],
            dst_ref=gbuf.at[m, at],
            send_sem=send_sem.at[m, c],
            recv_sem=recv_sem.at[m, c],
            device_id=((s + sections - 1) % sections, d),
            device_id_type=MESH,
        )

    def slot(m, carry):
        @pl.when(s < sections - 1)
        def _():
            for c in range(CHUNKS):
                hop(m, c).wait_recv()

        up_grad = fdot(up_ref[...], gbuf[m]).astype(jnp.bfloat16)
        ugbuf[...] = up_grad

        @pl.when(s > 0)
        def _():
            def chunk(c, carry):
                at = pl.ds(pl.multiple_of(c * rows, rows), rows)
                got = fdot(wbuf[at, :], gbuf[m]) + fdot(downt_ref[at, :], ugbuf[...])
                obuf[m, at, :] = got.astype(jnp.bfloat16)
                hop(m, c).start()
                return carry

            lax.fori_loop(0, CHUNKS, chunk, 0)

        inputs = abuf[pl.ds(pl.multiple_of(m * tokens, tokens), tokens), :]
        down_act = dabuf[:, pl.ds(pl.multiple_of(m * tokens, tokens), tokens)]
        down_term = fdot(ugbuf[...], inputs)
        up_term = fdot(down_act, gbuf[m], NT)
        tbuf[m, :rank, :] = down_term
        tbuf[m, rank:, :] = up_term
        square = jnp.sum(down_term * down_term + up_term * up_term, axis=0, keepdims=True)
        square = jnp.sum(square, axis=1, keepdims=True)
        sqbuf[pl.ds(m, 1), :] = jnp.broadcast_to(square, (1, LANES))
        return carry

    sqbuf[...] = jnp.zeros_like(sqbuf)
    redsend[:, features:] = jnp.zeros_like(redsend[:, features:])
    lax.fori_loop(0, slots, slot, 0)

    def sq_hop(k):
        return pltpu.make_async_remote_copy(
            src_ref=sqbuf, dst_ref=sqall.at[s],
            send_sem=sqs_sem.at[k], recv_sem=sqr_sem.at[k],
            device_id=((s + k) % sections, d), device_id_type=MESH,
        )

    for k in range(1, sections):
        sq_hop(k).start()
    sqall[s] = sqbuf[...]
    for k in range(1, sections):
        sq_hop(k).wait_recv()
    norm = jnp.sqrt(jnp.sum(sqall[...], axis=0))
    norm_ref[...] = norm
    factor = clip_scale / (norm + 0.01)
    total = factor[0:1, 0:1] * tbuf[0]
    for m in range(1, slots):
        total = total + factor[m : m + 1, 0:1] * tbuf[m]
    redsend[:, :features] = total.astype(jnp.bfloat16)

    def window_of(t):
        return pl.ds(pl.multiple_of(span * t // LANES * LANES, LANES), window)

    def red_hop(k):
        t = (d + k) % replicas
        return pltpu.make_async_remote_copy(
            src_ref=redsend.at[:, window_of(t)], dst_ref=redin.at[d],
            send_sem=rs_sem.at[k], recv_sem=rr_sem.at[k],
            device_id=(s, t), device_id_type=MESH,
        )

    for k in range(1, replicas):
        red_hop(k).start()
    redin[d] = redsend[:, window_of(d)]
    for k in range(1, replicas):
        red_hop(k).wait_recv()
    red_ref[...] = jnp.sum(redin[...].astype(jnp.float32), axis=0)

    @pl.when(s > 0)
    def _():
        def drain(m, carry):
            for c in range(CHUNKS):
                hop(m, c).wait_send()
            return carry

        lax.fori_loop(0, slots, drain, 0)

    for k in range(1, sections):
        sq_hop(k).wait_send()
    for k in range(1, replicas):
        red_hop(k).wait_send()


def on_device(acts, cotangent, frozen, down_adapter, up_adapter, example_ids, lengths):
    sections = lax.axis_size("section")
    replicas = lax.axis_size("dp")
    layer_inputs = acts[0]
    slots = example_ids.shape[1]
    features = layer_inputs.shape[1]
    tokens = layer_inputs.shape[0] // slots
    rank = down_adapter.shape[1]
    choose = (example_ids[0][:, None] == jnp.arange(slots, dtype=jnp.int32)[None, :]).astype(jnp.int32)
    slot_length = jnp.sum(choose * lengths[0][None, :], axis=1)
    live = (jnp.arange(tokens, dtype=jnp.int32)[None, :] < slot_length[:, None]).astype(jnp.bfloat16)
    seeded = cotangent.reshape(slots, tokens, features) * live[:, :, None]
    seeded = jnp.swapaxes(seeded, 1, 2)
    clip_scale = math.sqrt(2.0 * rank * features) / math.sqrt(replicas * slots)
    weight = lax.all_gather(frozen[0], "dp", axis=0, tiled=True)
    span = features // replicas
    window = -(-(span + LANES - 1) // LANES) * LANES
    vmem = pl.BlockSpec(memory_space=pltpu.VMEM)
    hbm = pl.BlockSpec(memory_space=pl.ANY)
    dma = pltpu.SemaphoreType.DMA
    bf16, f32 = jnp.bfloat16, jnp.float32
    reduced, norms = pl.pallas_call(
        functools.partial(kernel, sections, replicas, clip_scale),
        out_shape=(
            jax.ShapeDtypeStruct((2 * rank, window), f32),
            jax.ShapeDtypeStruct((8, LANES), f32),
        ),
        in_specs=[hbm, hbm, hbm, vmem, vmem, vmem],
        out_specs=(vmem, vmem),
        scratch_shapes=[
            pltpu.VMEM((features, features), bf16),
            pltpu.VMEM((slots, features, tokens), bf16),
            pltpu.VMEM((slots, features, tokens), bf16),
            pltpu.VMEM((slots * tokens, features), bf16),
            pltpu.VMEM((rank, tokens), bf16),
            pltpu.VMEM((rank, slots * tokens), bf16),
            pltpu.VMEM((slots, 2 * rank, features), f32),
            pltpu.VMEM((8, LANES), f32),
            pltpu.VMEM((sections, 8, LANES), f32),
            pltpu.VMEM((2 * rank, features + LANES), bf16),
            pltpu.VMEM((replicas, 2 * rank, window), bf16),
            dma((CHUNKS,)), dma, dma,
            dma((slots, CHUNKS)), dma((slots, CHUNKS)),
            dma((sections,)), dma((sections,)),
            dma((replicas,)), dma((replicas,)),
        ],
        compiler_params=pltpu.CompilerParams(
            collective_id=0, has_side_effects=True, vmem_limit_bytes=60 * 1024 * 1024
        ),
    )(weight, seeded, layer_inputs, up_adapter[0], down_adapter[0], down_adapter[0].T)
    shift = span * lax.axis_index("dp") % LANES
    mine = lax.dynamic_slice_in_dim(reduced, shift, span, axis=1)
    slot_norms = norms[:slots, 0]
    example_norms = jnp.sum(choose.astype(f32) * slot_norms[:, None], axis=0)
    return (mine[None, :rank], mine[None, rank:], example_norms[None])


def solution(mesh):
    in_specs = (
        P("section", "dp", None),
        P("dp", None),
        P("section", "dp", None),
        P("section", None, None),
        P("section", None, None),
        P("dp", None),
        P("dp", None),
    )
    out_specs = (P("section", None, "dp"), P("section", None, "dp"), P("dp", None))
    return jax.shard_map(
        on_device, mesh=mesh, in_specs=in_specs, out_specs=out_specs, check_vma=False
    )
```

```python
import functools
import math

import jax
import jax.numpy as jnp
from jax import lax
from jax.experimental import pallas as pl
from jax.experimental.pallas import tpu as pltpu
from jax.sharding import PartitionSpec as P

MESH = pl.DeviceIdType.MESH
NT = (((1,), (1,)), ((), ()))
LANES = 128
SIDE = 4
SUBS = 4
QUADS = 4


def fdot(a, b, dims=None):
    if dims is None:
        return jnp.dot(a, b, preferred_element_type=jnp.float32)
    return lax.dot_general(a, b, dims, preferred_element_type=jnp.float32)


def kernel(
    sections, replicas, slots, clip_scale,
    frozen_hbm, cot_hbm, acts_hbm, up_ref, down_ref, live_ref,
    red_ref, norm_ref,
    wbuf, gbuf, obuf, abuf, cbuf, upb, downb, dtb, ugb, dab, tbuf, sqbuf, sqall, redsend, redin,
    local_sem, swap_send, swap_recv, ws, wr, es, er, ys, yr, fs, fr, sqs, sqr, rs, rr,
):
    s = lax.axis_index("section")
    d = lax.axis_index("dp")
    y, c = s // 2, s % 2
    top = y == sections // 2 - 1
    half = wbuf.shape[2]
    features = wbuf.shape[3]
    width = gbuf.shape[4]
    tokens = width // slots
    rank = up_ref.shape[0]
    span = features // replicas
    window = redin.shape[2]
    cols = features // SUBS
    group = replicas // QUADS
    partner = s + 1 - 2 * c
    below = (s + sections - 2) % sections
    mine = 1 - c

    z, x = d // SIDE, d % SIDE
    q = (x + 1) % SIDE
    p = (1 - c) * (SIDE * z + (z + x) % SIDE) + c * (SIDE * q + (z + q + 3) % SIDE)

    def device_at(pos):
        pos = (pos + 2 * replicas) % replicas
        hi, lo = pos // SIDE, pos % SIDE
        first = SIDE * hi + (lo + SIDE - hi) % SIDE
        second = SIDE * ((lo + 1 + SIDE - hi) % SIDE) + (hi + 3) % SIDE
        return (1 - c) * first + c * second

    def remote(src, dst, send, recv, device):
        return pltpu.make_async_remote_copy(
            src_ref=src, dst_ref=dst, send_sem=send, recv_sem=recv,
            device_id=device, device_id_type=MESH,
        )

    barrier = pltpu.get_barrier_semaphore()
    for k in range(1, sections):
        pl.semaphore_signal(barrier, inc=1, device_id=((s + k) % sections, d), device_id_type=MESH)
    for k in range(1, replicas):
        pl.semaphore_signal(barrier, inc=1, device_id=(s, (d + k) % replicas), device_id_type=MESH)

    def half_rows(h):
        return frozen_hbm.at[pl.ds(pl.multiple_of(h * half, 16), half)]

    own_copy = pltpu.make_async_copy(half_rows(c), wbuf.at[mine, d], local_sem.at[0])
    acts_copy = pltpu.make_async_copy(acts_hbm, abuf, local_sem.at[1])
    cot_copy = pltpu.make_async_copy(cot_hbm, cbuf, local_sem.at[2])
    own_copy.start()
    acts_copy.start()

    @pl.when(top)
    def _():
        cot_copy.start()

    upb[mine] = up_ref[...]
    downb[mine] = down_ref[...]
    sqbuf[...] = jnp.zeros_like(sqbuf)
    redsend[:, features:] = jnp.zeros_like(redsend[:, features:])
    pl.semaphore_wait(barrier, sections - 1 + replicas - 1)

    def swaps(j):
        to = (partner, d)
        return (
            remote(half_rows(1 - c), wbuf.at[j, d], swap_send.at[0], swap_recv.at[0], to),
            remote(up_ref, upb.at[j], swap_send.at[1], swap_recv.at[1], to),
            remote(down_ref, downb.at[j], swap_send.at[2], swap_recv.at[2], to),
        )

    for copy in swaps(mine):
        copy.start()
    own_copy.wait()
    for copy in swaps(c):
        copy.wait_recv()

    def ring(j, way, k, sub, origin):
        at = wbuf.at[j, device_at(origin), :, pl.ds(pl.multiple_of(sub * cols, LANES), cols)]
        to = (s, device_at(p + 1 - 2 * way))
        return remote(at, at, ws.at[j, way, k - 1, sub], wr.at[j, way, k - 1, sub], to)

    def sending(j, way, k, sub):
        return ring(j, way, k, sub, p - (1 - 2 * way) * (k - 1))

    def arriving(j, way, k, sub):
        return ring(j, way, k, sub, p - (1 - 2 * way) * k)

    last = replicas // 2

    def begin(j):
        for sub in range(SUBS):
            for way in range(2):
                sending(j, way, 1, sub).start()

    def serve(j, k, sub):
        for way in range(2):
            ours = (sub < SUBS // 2) if way == 0 else (sub >= SUBS // 2)

            @pl.when((k < last) | ours)
            def _(way=way):
                arriving(j, way, k, sub).wait_recv()

            @pl.when((k < last - 1) | ((k == last - 1) & ours))
            def _(way=way):
                sending(j, way, k + 1, sub).start()

    def waves(j, first, count, work=None):
        def wave(w, carry):
            serve(j, first + w // SUBS, w % SUBS)
            if work is not None:
                work(w)
            return carry

        lax.fori_loop(0, count, wave, 0)

    def lanes(m):
        return pl.ds(pl.multiple_of(m * tokens, LANES), tokens)

    def seed(w):
        @pl.when(top)
        def _():
            m, part = w // QUADS, w % QUADS
            wide = features // QUADS
            block = cbuf[
                pl.ds(pl.multiple_of(m * tokens, tokens), tokens),
                pl.ds(pl.multiple_of(part * wide, LANES), wide),
            ]
            turned = block.astype(jnp.float32).T * live_ref[0:1, lanes(m)]
            gbuf[0, pl.ds(part * group, group), :, :, lanes(m)] = turned.astype(jnp.bfloat16).reshape(
                group, 2, half, tokens
            )

    begin(0)

    @pl.when(top)
    def _():
        cot_copy.wait()

    waves(0, 1, 16, seed)
    acts_copy.wait()
    dab[...] = fdot(down_ref[...], abuf[...], NT).astype(jnp.bfloat16)
    for j in range(2):
        turned = downb[j].astype(jnp.float32).T
        dtb[j] = turned.astype(jnp.bfloat16).reshape(replicas, 2, half, rank)

    def whole(j):
        return gbuf[j].reshape(features, width)

    def part_of(j, m):
        return gbuf[j, :, :, :, lanes(m)].reshape(features, tokens)

    @pl.when(top)
    def _():
        ugb[0] = fdot(upb[0], whole(0)).astype(jnp.bfloat16)

    waves(0, 5, 12)
    begin(1)
    waves(0, 8, 4)

    def top_product(j, o):
        got = fdot(wbuf[j, o], whole(j)) + fdot(dtb[j, o, c], ugb[j])
        return got.astype(jnp.bfloat16)

    def across(o):
        at = gbuf.at[1, o, c]
        return remote(at, at, es.at[o], er.at[o], (partner, d))

    def across_in(o):
        at = gbuf.at[1, o, 1 - c]
        return remote(at, at, es.at[o], er.at[o], (partner, d))

    def down_hop(o):
        return remote(obuf.at[o], gbuf.at[0, o, c], ys.at[o], yr.at[o], (below, d))

    def relay(o):
        at = gbuf.at[0, o, c]
        return remote(at, at, fs.at[o], fr.at[o], (partner, d))

    def relay_in(o):
        at = gbuf.at[0, o, 1 - c]
        return remote(at, at, fs.at[o], fr.at[o], (partner, d))

    def block_at(r):
        return device_at(p - (r % 2) * ((r + 1) // 2) + (1 - r % 2) * (r // 2))

    def upper(w):
        @pl.when(top)
        def _():
            def one(i, carry):
                o = 2 * w + i
                gbuf[1, o, c] = top_product(0, o)
                across(o).start()
                return carry

            lax.fori_loop(0, 2, one, 0)

    def lower(r):
        o = block_at(r)
        obuf[o] = top_product(1, o)
        down_hop(o).start()

    def hand_on(r):
        o = block_at(r)
        down_hop_in(o).wait_recv()
        relay(o).start()

    def down_hop_in(o):
        return remote(obuf.at[o], gbuf.at[0, o, c], ys.at[o], yr.at[o], (below, d))

    waves(1, 1, 8, upper)

    @pl.when(top)
    def _():
        def one(o, carry):
            across_in(o).wait_recv()
            return carry

        lax.fori_loop(0, replicas, one, 0)
        ugb[1] = fdot(upb[1], whole(1)).astype(jnp.bfloat16)

    second = y == sections // 2 - 2

    def middle(w):
        @pl.when(top & ((w < 4) | (w % 2 == 0)))
        def _():
            lower(jnp.where(w < 4, w, 2 + w // 2))

        @pl.when(second & (w >= 4) & (w % 2 == 1))
        def _():
            hand_on((w - 4) // 2)

    waves(1, 3, 20, middle)

    def final(w):
        @pl.when(top)
        def _():
            lower(12 + w)

    def final_three(w):
        @pl.when(top & (w < 3))
        def _():
            lower(12 + w)

    waves(1, 8, 4, final_three)

    @pl.when(top)
    def _():
        lower(15)

    @pl.when(second)
    def _():
        def one(r, carry):
            hand_on(r)
            return carry

        lax.fori_loop(8, replicas, one, 0)

        def two(o, carry):
            relay_in(o).wait_recv()
            return carry

        lax.fori_loop(0, replicas, two, 0)

    def terms(m):
        inputs = abuf[pl.ds(pl.multiple_of(m * tokens, tokens), tokens), :]
        down_term = fdot(ugb[mine, :, lanes(m)], inputs)
        up_term = fdot(dab[:, lanes(m)], part_of(mine, m), NT)
        tbuf[m, :rank, :] = down_term
        tbuf[m, rank:, :] = up_term
        square = jnp.sum(down_term * down_term + up_term * up_term, axis=0, keepdims=True)
        square = jnp.sum(square, axis=1, keepdims=True)
        sqbuf[pl.ds(m, 1), :] = jnp.broadcast_to(square, (1, LANES))

    def quad(ref, j, m, part, side):
        return ref.at[j, pl.ds(part * group, group), side, :, lanes(m)]

    def quad_product(j, m, part):
        blocks = pl.ds(part * group, group)
        weight = wbuf[j, blocks].reshape(group * half, features)
        adapter = dtb[j, blocks, c].reshape(group * half, rank)
        got = fdot(weight, part_of(j, m)) + fdot(adapter, ugb[j, :, lanes(m)])
        return got.astype(jnp.bfloat16).reshape(group, half, tokens)

    def quad_across(m, part, side):
        at = quad(gbuf, 1, m, part, side)
        return remote(at, at, es.at[m * QUADS + part], er.at[m * QUADS + part], (partner, d))

    def quad_down(m, part):
        src = obuf.at[pl.ds(part * group, group), :, lanes(m)]
        at = m * QUADS + part
        return remote(src, quad(gbuf, 0, m, part, c), ys.at[at], yr.at[at], (below, d))

    def quad_relay(m, part, side):
        at = quad(gbuf, 0, m, part, side)
        return remote(at, at, fs.at[m * QUADS + part], fr.at[m * QUADS + part], (partner, d))

    def each_quad(work):
        def one(part, carry):
            work(part)
            return carry

        lax.fori_loop(0, QUADS, one, 0)

    def slot(m, carry):
        @pl.when(y < sections // 2 - 2)
        def _():
            def pass_on(part):
                quad_down(m, part).wait_recv()
                quad_relay(m, part, c).start()

            each_quad(pass_on)
            each_quad(lambda part: quad_relay(m, part, 1 - c).wait_recv())

        ugb[0, :, lanes(m)] = fdot(upb[0], part_of(0, m)).astype(jnp.bfloat16)

        def odd(part):
            gbuf[1, pl.ds(part * group, group), c, :, lanes(m)] = quad_product(0, m, part)
            quad_across(m, part, c).start()

        each_quad(odd)

        @pl.when(c == 1)
        def _():
            terms(m)

        each_quad(lambda part: quad_across(m, part, 1 - c).wait_recv())
        ugb[1, :, lanes(m)] = fdot(upb[1], part_of(1, m)).astype(jnp.bfloat16)

        @pl.when(y > 0)
        def _():
            def even(part):
                obuf[pl.ds(part * group, group), :, lanes(m)] = quad_product(1, m, part)
                quad_down(m, part).start()

            each_quad(even)

        @pl.when(c == 0)
        def _():
            terms(m)

        return carry

    @pl.when(y < sections // 2 - 1)
    def _():
        lax.fori_loop(0, slots, slot, 0)

    @pl.when(top)
    def _():
        def one(m, carry):
            terms(m)
            return carry

        lax.fori_loop(0, slots, one, 0)

    def sq_hop(k):
        return remote(sqbuf, sqall.at[s], sqs.at[k], sqr.at[k], ((s + k) % sections, d))

    for k in range(1, sections):
        sq_hop(k).start()
    sqall[s] = sqbuf[...]
    for k in range(1, sections):
        sq_hop(k).wait_recv()
    norm = jnp.sqrt(jnp.sum(sqall[...], axis=0))
    norm_ref[...] = norm
    factor = clip_scale / (norm + 0.01)
    total = factor[0:1, 0:1] * tbuf[0]
    for m in range(1, slots):
        total = total + factor[m : m + 1, 0:1] * tbuf[m]
    redsend[:, :features] = total.astype(jnp.bfloat16)

    def window_of(t):
        return pl.ds(pl.multiple_of(span * t // LANES * LANES, LANES), window)

    def red_hop(k):
        t = (d + k) % replicas
        return remote(redsend.at[:, window_of(t)], redin.at[d], rs.at[k], rr.at[k], (s, t))

    for k in range(1, replicas):
        red_hop(k).start()
    redin[d] = redsend[:, window_of(d)]
    for k in range(1, replicas):
        red_hop(k).wait_recv()
    red_ref[...] = jnp.sum(redin[...].astype(jnp.float32), axis=0)

    for copy in swaps(mine):
        copy.wait_send()
    for j in range(2):

        def one(w, carry):
            k, sub = 1 + w // SUBS, w % SUBS
            for way in range(2):
                ours = (sub < SUBS // 2) if way == 0 else (sub >= SUBS // 2)

                @pl.when((k < last) | ours)
                def _(way=way):
                    sending(j, way, k, sub).wait_send()

            return carry

        lax.fori_loop(0, last * SUBS, one, 0)

    @pl.when(top)
    def _():
        def one(o, carry):
            across(o).wait_send()
            down_hop(o).wait_send()
            return carry

        lax.fori_loop(0, replicas, one, 0)

    @pl.when(second)
    def _():
        def one(o, carry):
            relay(o).wait_send()
            return carry

        lax.fori_loop(0, replicas, one, 0)

    @pl.when(y < sections // 2 - 1)
    def _():
        def one(w, carry):
            m, part = w // QUADS, w % QUADS
            quad_across(m, part, c).wait_send()

            @pl.when(y > 0)
            def _():
                quad_down(m, part).wait_send()

            @pl.when(y < sections // 2 - 2)
            def _():
                quad_relay(m, part, c).wait_send()

            return carry

        lax.fori_loop(0, slots * QUADS, one, 0)

    for k in range(1, sections):
        sq_hop(k).wait_send()
    for k in range(1, replicas):
        red_hop(k).wait_send()


def on_device(acts, cotangent, frozen, down_adapter, up_adapter, example_ids, lengths):
    sections = lax.axis_size("section")
    replicas = lax.axis_size("dp")
    layer_inputs = acts[0]
    slots = example_ids.shape[1]
    width, features = layer_inputs.shape
    tokens = width // slots
    rank = down_adapter.shape[1]
    choose = (example_ids[0][:, None] == jnp.arange(slots, dtype=jnp.int32)[None, :]).astype(jnp.int32)
    slot_length = jnp.sum(choose * lengths[0][None, :], axis=1)
    live = (jnp.arange(tokens, dtype=jnp.int32)[None, :] < slot_length[:, None]).astype(jnp.float32)
    live = jnp.broadcast_to(live.reshape(1, width), (8, width))
    clip_scale = math.sqrt(2.0 * rank * features) / math.sqrt(replicas * slots)
    span = features // replicas
    half = span // 2
    window = -(-(span + LANES - 1) // LANES) * LANES
    vmem = pl.BlockSpec(memory_space=pltpu.VMEM)
    hbm = pl.BlockSpec(memory_space=pl.ANY)
    dma = pltpu.SemaphoreType.DMA
    bf16, f32 = jnp.bfloat16, jnp.float32
    reduced, norms = pl.pallas_call(
        functools.partial(kernel, sections, replicas, slots, clip_scale),
        out_shape=(
            jax.ShapeDtypeStruct((2 * rank, window), f32),
            jax.ShapeDtypeStruct((8, LANES), f32),
        ),
        in_specs=[hbm, hbm, hbm, vmem, vmem, vmem],
        out_specs=(vmem, vmem),
        scratch_shapes=[
            pltpu.VMEM((2, replicas, half, features), bf16),
            pltpu.VMEM((2, replicas, 2, half, width), bf16),
            pltpu.VMEM((replicas, half, width), bf16),
            pltpu.VMEM((width, features), bf16),
            pltpu.VMEM((width, features), bf16),
            pltpu.VMEM((2, rank, features), bf16),
            pltpu.VMEM((2, rank, features), bf16),
            pltpu.VMEM((2, replicas, 2, half, rank), bf16),
            pltpu.VMEM((2, rank, width), bf16),
            pltpu.VMEM((rank, width), bf16),
            pltpu.VMEM((slots, 2 * rank, features), f32),
            pltpu.VMEM((8, LANES), f32),
            pltpu.VMEM((sections, 8, LANES), f32),
            pltpu.VMEM((2 * rank, features + LANES), bf16),
            pltpu.VMEM((replicas, 2 * rank, window), bf16),
            dma((3,)), dma((3,)), dma((3,)),
            dma((2, 2, replicas // 2, SUBS)), dma((2, 2, replicas // 2, SUBS)),
            dma((replicas,)), dma((replicas,)),
            dma((replicas,)), dma((replicas,)),
            dma((replicas,)), dma((replicas,)),
            dma((sections,)), dma((sections,)),
            dma((replicas,)), dma((replicas,)),
        ],
        compiler_params=pltpu.CompilerParams(
            collective_id=0, has_side_effects=True, vmem_limit_bytes=62 * 1024 * 1024
        ),
    )(frozen[0], cotangent, layer_inputs, up_adapter[0], down_adapter[0], live)
    shift = span * lax.axis_index("dp") % LANES
    mine = lax.dynamic_slice_in_dim(reduced, shift, span, axis=1)
    slot_norms = norms[:slots, 0]
    example_norms = jnp.sum(choose.astype(f32) * slot_norms[:, None], axis=0)
    return (mine[None, :rank], mine[None, rank:], example_norms[None])


def solution(mesh):
    in_specs = (
        P("section", "dp", None),
        P("dp", None),
        P("section", "dp", None),
        P("section", None, None),
        P("section", None, None),
        P("dp", None),
        P("dp", None),
    )
    out_specs = (P("section", None, "dp"), P("section", None, "dp"), P("dp", None))
    return jax.shard_map(
        on_device, mesh=mesh, in_specs=in_specs, out_specs=out_specs, check_vma=False
    )
```

```python
import functools
import math

import jax
import jax.numpy as jnp
from jax import lax
from jax.experimental import pallas as pl
from jax.experimental.pallas import tpu as pltpu
from jax.sharding import PartitionSpec as P

MESH = pl.DeviceIdType.MESH
NT = (((1,), (1,)), ((), ()))
LANES = 128
SIDE = 4
SUBS = 4
QUADS = 4


def fdot(a, b, dims=None):
    if dims is None:
        return jnp.dot(a, b, preferred_element_type=jnp.float32)
    return lax.dot_general(a, b, dims, preferred_element_type=jnp.float32)


def kernel(
    sections, replicas, slots, clip_scale,
    frozen_hbm, cot_hbm, acts_hbm, up_ref, down_ref, ids_ref, lengths_ref,
    out_ref,
    wbuf, gbuf, obuf, abuf, cbuf, upb, downb, dtb, ugb, dab, tbuf, sqbuf, sqall, redsend, redin,
    live,
    local_sem, swap_send, swap_recv, ws, wr, es, er, ys, yr, fs, fr, sqs, sqr, rs, rr,
    y2s, y2r, f2s, f2r,
):
    s = lax.axis_index("section")
    d = lax.axis_index("dp")
    y, c = s // 2, s % 2
    top = y == sections // 2 - 1
    half = wbuf.shape[2]
    features = wbuf.shape[3]
    width = gbuf.shape[4]
    tokens = width // slots
    rank = up_ref.shape[0]
    span = features // replicas
    window = redin.shape[2]
    cols = features // SUBS
    group = replicas // QUADS
    partner = s + 1 - 2 * c
    below = (s + sections - 2) % sections
    mine = 1 - c

    z, x = d // SIDE, d % SIDE
    q = (x + 1) % SIDE
    p = (1 - c) * (SIDE * z + (z + x) % SIDE) + c * (SIDE * q + (z + q + 3) % SIDE)

    def device_at(pos):
        pos = (pos + 2 * replicas) % replicas
        hi, lo = pos // SIDE, pos % SIDE
        first = SIDE * hi + (lo + SIDE - hi) % SIDE
        second = SIDE * ((lo + 1 + SIDE - hi) % SIDE) + (hi + 3) % SIDE
        return (1 - c) * first + c * second

    p2 = c * (SIDE * z + (z + x) % SIDE) + (1 - c) * (SIDE * q + (z + q + 3) % SIDE)

    def other_device_at(pos):
        pos = (pos + 2 * replicas) % replicas
        hi, lo = pos // SIDE, pos % SIDE
        first = SIDE * hi + (lo + SIDE - hi) % SIDE
        second = SIDE * ((lo + 1 + SIDE - hi) % SIDE) + (hi + 3) % SIDE
        return c * first + (1 - c) * second

    def remote(src, dst, send, recv, device):
        return pltpu.make_async_remote_copy(
            src_ref=src, dst_ref=dst, send_sem=send, recv_sem=recv,
            device_id=device, device_id_type=MESH,
        )

    barrier = pltpu.get_barrier_semaphore()
    for k in range(1, sections):
        pl.semaphore_signal(barrier, inc=1, device_id=((s + k) % sections, d), device_id_type=MESH)
    for k in range(1, replicas):
        pl.semaphore_signal(barrier, inc=1, device_id=(s, (d + k) % replicas), device_id_type=MESH)

    def half_rows(h):
        return frozen_hbm.at[pl.ds(pl.multiple_of(h * half, 16), half)]

    own_copy = pltpu.make_async_copy(half_rows(c), wbuf.at[mine, d], local_sem.at[0])
    acts_copy = pltpu.make_async_copy(acts_hbm, abuf, local_sem.at[1])
    cot_copy = pltpu.make_async_copy(cot_hbm, cbuf, local_sem.at[2])
    own_copy.start()
    acts_copy.start()

    @pl.when(top)
    def _():
        cot_copy.start()

    place = lax.broadcasted_iota(jnp.int32, (8, tokens), 1)
    for m in range(slots):
        length = jnp.int32(0)
        for k in range(slots):
            length = length + jnp.where(ids_ref[0, m] == k, lengths_ref[0, k], 0)
        live[:, m * tokens : (m + 1) * tokens] = jnp.where(place < length, 1.0, 0.0)
    upb[mine] = up_ref[...]
    downb[mine] = down_ref[...]
    sqbuf[...] = jnp.zeros_like(sqbuf)
    redsend[:, features:] = jnp.zeros_like(redsend[:, features:])
    pl.semaphore_wait(barrier, sections - 1 + replicas - 1)

    def swaps(j):
        to = (partner, d)
        return (
            remote(half_rows(1 - c), wbuf.at[j, d], swap_send.at[0], swap_recv.at[0], to),
            remote(up_ref, upb.at[j], swap_send.at[1], swap_recv.at[1], to),
            remote(down_ref, downb.at[j], swap_send.at[2], swap_recv.at[2], to),
        )

    for copy in swaps(mine):
        copy.start()
    own_copy.wait()

    def swapped():
        for copy in swaps(c):
            copy.wait_recv()

    def ring(j, way, k, sub, origin):
        at = wbuf.at[j, device_at(origin), :, pl.ds(pl.multiple_of(sub * cols, LANES), cols)]
        to = (s, device_at(p + 1 - 2 * way))
        return remote(at, at, ws.at[j, way, k - 1, sub], wr.at[j, way, k - 1, sub], to)

    def sending(j, way, k, sub):
        return ring(j, way, k, sub, p - (1 - 2 * way) * (k - 1))

    def arriving(j, way, k, sub):
        return ring(j, way, k, sub, p - (1 - 2 * way) * k)

    last = replicas // 2

    def begin(j):
        for sub in range(SUBS):
            for way in range(2):
                sending(j, way, 1, sub).start()

    def serve(j, k, sub):
        for way in range(2):
            ours = (sub < SUBS // 2) if way == 0 else (sub >= SUBS // 2)

            @pl.when((k < last) | ours)
            def _(way=way):
                arriving(j, way, k, sub).wait_recv()

            @pl.when((k < last - 1) | ((k == last - 1) & ours))
            def _(way=way):
                sending(j, way, k + 1, sub).start()

    def waves(j, first, count, work=None):
        def wave(w, carry):
            serve(j, first + w // SUBS, w % SUBS)
            if work is not None:
                work(w)
            return carry

        lax.fori_loop(0, count, wave, 0)

    def lanes(m):
        return pl.ds(pl.multiple_of(m * tokens, LANES), tokens)

    def seed(w):
        @pl.when(top)
        def _():
            m, part = w // QUADS, w % QUADS
            wide = features // QUADS
            block = cbuf[
                pl.ds(pl.multiple_of(m * tokens, tokens), tokens),
                pl.ds(pl.multiple_of(part * wide, LANES), wide),
            ]
            turned = block.astype(jnp.float32).T * live[0:1, lanes(m)]
            gbuf[0, pl.ds(part * group, group), :, :, lanes(m)] = turned.astype(jnp.bfloat16).reshape(
                group, 2, half, tokens
            )

    @pl.when(c == 0)
    def _():
        swapped()

    begin(0)

    @pl.when(c == 1)
    def _():
        swapped()


    @pl.when(top)
    def _():
        cot_copy.wait()

    waves(0, 1, 16, seed)
    acts_copy.wait()
    dab[...] = fdot(down_ref[...], abuf[...], NT).astype(jnp.bfloat16)
    for j in range(2):
        turned = downb[j].astype(jnp.float32).T
        dtb[j] = turned.astype(jnp.bfloat16).reshape(replicas, 2, half, rank)

    def whole(j):
        return gbuf[j].reshape(features, width)

    def part_of(j, m):
        return gbuf[j, :, :, :, lanes(m)].reshape(features, tokens)

    @pl.when(top)
    def _():
        ugb[0] = fdot(upb[0], whole(0)).astype(jnp.bfloat16)

    waves(0, 5, 12)
    begin(1)
    waves(0, 8, 4)

    def top_product(j, o):
        got = fdot(wbuf[j, o], whole(j)) + fdot(dtb[j, o, c], ugb[j])
        return got.astype(jnp.bfloat16)

    def across(o):
        at = gbuf.at[1, o, c]
        return remote(at, at, es.at[o], er.at[o], (partner, d))

    def across_in(o):
        at = gbuf.at[1, o, 1 - c]
        return remote(at, at, es.at[o], er.at[o], (partner, d))

    def down_hop(o):
        return remote(obuf.at[o], gbuf.at[0, o, c], ys.at[o], yr.at[o], (below, d))

    def relay(o):
        at = gbuf.at[0, o, c]
        return remote(at, at, fs.at[o], fr.at[o], (partner, d))

    def relay_in(o):
        at = gbuf.at[0, o, 1 - c]
        return remote(at, at, fs.at[o], fr.at[o], (partner, d))

    def block_at(r):
        return device_at(p - (r % 2) * ((r + 1) // 2) + (1 - r % 2) * (r // 2))

    def other_block_at(r):
        return other_device_at(p2 - (r % 2) * ((r + 1) // 2) + (1 - r % 2) * (r // 2))

    def upper(w):
        @pl.when(top)
        def _():
            def one(i, carry):
                o = 2 * w + i
                gbuf[1, o, c] = top_product(0, o)
                across(o).start()
                return carry

            lax.fori_loop(0, 2, one, 0)

    def lower(r):
        o = block_at(r)
        obuf[o] = top_product(1, o)
        down_hop(o).start()

    def hand_on(r):
        o = block_at(r)
        down_hop(o).wait_recv()
        relay(o).start()

    waves(1, 1, 8, upper)

    @pl.when(top)
    def _():
        def one(o, carry):
            across_in(o).wait_recv()
            return carry

        lax.fori_loop(0, replicas, one, 0)
        ugb[1] = fdot(upb[1], whole(1)).astype(jnp.bfloat16)

    second = y == sections // 2 - 2

    def middle(w):
        early, step, turn = w < 7, w // SUBS, w % SUBS

        @pl.when(top & (early | ((w >= 8) & (turn % 2 == 0))))
        def _():
            lower(jnp.where(early, w, 3 + 2 * step + turn // 2))

        @pl.when(second & (w >= 4) & (w % 2 == 1))
        def _():
            hand_on((w - 4) // 2)

    waves(1, 3, 20, middle)

    def late_hop(i, m):
        o = block_at(replicas - 2 + i)
        dst = gbuf.at[0, o, c, :, lanes(m)]
        return remote(obuf.at[o, :, lanes(m)], dst, y2s.at[i, m], y2r.at[i, m], (below, d))

    def late_relay(i, m, side):
        o = block_at(replicas - 2 + i)
        if side == 1:
            o = other_block_at(replicas - 2 + i)
        at = gbuf.at[0, o, c if side == 0 else 1 - c, :, lanes(m)]
        return remote(at, at, f2s.at[i, m], f2r.at[i, m], (partner, d))

    def final(w):
        @pl.when(top & (w == 0))
        def _():
            lower(13)

        @pl.when(top & (w == 1))
        def _():
            o = block_at(14)
            obuf[o] = top_product(1, o)
            late_hop(0, 0).start()

        @pl.when(second & (w < 3))
        def _():
            hand_on(8 + w)

    waves(1, 8, 4, final)

    @pl.when(top)
    def _():
        o = block_at(15)
        obuf[o] = top_product(1, o)
        late_hop(1, 0).start()
        for m in range(1, slots):
            for i in range(2):
                late_hop(i, m).start()

    @pl.when(second)
    def _():
        def one(r, carry):
            hand_on(r)
            return carry

        lax.fori_loop(11, replicas - 2, one, 0)

        def two(r, carry):
            relay_in(other_block_at(r)).wait_recv()
            return carry

        lax.fori_loop(0, replicas - 2, two, 0)

    def terms(m):
        inputs = abuf[pl.ds(pl.multiple_of(m * tokens, tokens), tokens), :]
        down_term = fdot(ugb[mine, :, lanes(m)], inputs)
        up_term = fdot(dab[:, lanes(m)], part_of(mine, m), NT)
        tbuf[m, :rank, :] = down_term
        tbuf[m, rank:, :] = up_term
        square = jnp.sum(down_term * down_term + up_term * up_term, axis=0, keepdims=True)
        square = jnp.sum(square, axis=1, keepdims=True)
        sqbuf[pl.ds(m, 1), :] = jnp.broadcast_to(square, (1, LANES))

    def quad(ref, j, m, part, side):
        return ref.at[j, pl.ds(part * group, group), side, :, lanes(m)]

    def quad_product(j, m, part):
        blocks = pl.ds(part * group, group)
        weight = wbuf[j, blocks].reshape(group * half, features)
        adapter = dtb[j, blocks, c].reshape(group * half, rank)
        got = fdot(weight, part_of(j, m)) + fdot(adapter, ugb[j, :, lanes(m)])
        return got.astype(jnp.bfloat16).reshape(group, half, tokens)

    def quad_across(m, part, side):
        at = quad(gbuf, 1, m, part, side)
        return remote(at, at, es.at[m * QUADS + part], er.at[m * QUADS + part], (partner, d))

    def quad_down(m, part):
        src = obuf.at[pl.ds(part * group, group), :, lanes(m)]
        at = m * QUADS + part
        return remote(src, quad(gbuf, 0, m, part, c), ys.at[at], yr.at[at], (below, d))

    def quad_relay(m, part, side):
        at = quad(gbuf, 0, m, part, side)
        return remote(at, at, fs.at[m * QUADS + part], fr.at[m * QUADS + part], (partner, d))

    def each_quad(work):
        def one(part, carry):
            work(part)
            return carry

        lax.fori_loop(0, QUADS, one, 0)

    def odd_whole(m):
        ugb[0, :, lanes(m)] = fdot(upb[0], part_of(0, m)).astype(jnp.bfloat16)

        def odd(part):
            gbuf[1, pl.ds(part * group, group), c, :, lanes(m)] = quad_product(0, m, part)
            quad_across(m, part, c).start()

        each_quad(odd)

    def slot(m, carry):
        @pl.when(second)
        def _():
            for i in range(2):
                late_hop(i, m).wait_recv()
                late_relay(i, m, 0).start()
            for i in range(2):
                late_relay(i, m, 1).wait_recv()
            odd_whole(m)

        @pl.when(y < sections // 2 - 2)
        def _():
            def pass_on(part):
                quad_down(m, part).wait_recv()
                quad_relay(m, part, c).start()

            each_quad(pass_on)
            each_quad(lambda part: quad_relay(m, part, 1 - c).wait_recv())
            odd_whole(m)

        @pl.when(c == 1)
        def _():
            terms(m)

        @pl.when((c == 0) & (m > 0))
        def _():
            terms(m - 1)

        each_quad(lambda part: quad_across(m, part, 1 - c).wait_recv())
        ugb[1, :, lanes(m)] = fdot(upb[1], part_of(1, m)).astype(jnp.bfloat16)

        @pl.when(y > 0)
        def _():
            def even(part):
                obuf[pl.ds(part * group, group), :, lanes(m)] = quad_product(1, m, part)
                quad_down(m, part).start()

            each_quad(even)

        return carry

    @pl.when(y < sections // 2 - 1)
    def _():
        lax.fori_loop(0, slots, slot, 0)

        @pl.when(c == 0)
        def _():
            terms(slots - 1)

    @pl.when(top)
    def _():
        def one(m, carry):
            terms(m)
            return carry

        lax.fori_loop(0, slots, one, 0)

    def sq_hop(k):
        return remote(sqbuf, sqall.at[s], sqs.at[k], sqr.at[k], ((s + k) % sections, d))

    for k in range(1, sections):
        sq_hop(k).start()
    sqall[s] = sqbuf[...]
    for k in range(1, sections):
        sq_hop(k).wait_recv()
    norm = jnp.sqrt(jnp.sum(sqall[...], axis=0))
    lane = lax.broadcasted_iota(jnp.int32, (1, LANES), 1)
    named = jnp.zeros((1, LANES), jnp.float32)
    for m in range(slots):
        named = named + jnp.where(lane == ids_ref[0, m], norm[m : m + 1, :], 0.0)
    out_ref[2 * rank :, :LANES] = jnp.broadcast_to(named, (8, LANES))
    out_ref[2 * rank :, LANES:] = jnp.zeros((8, window - LANES), jnp.float32)
    factor = clip_scale / (norm + 0.01)
    total = factor[0:1, 0:1] * tbuf[0]
    for m in range(1, slots):
        total = total + factor[m : m + 1, 0:1] * tbuf[m]
    redsend[:, :features] = total.astype(jnp.bfloat16)

    def window_of(t):
        return pl.ds(pl.multiple_of(span * t // LANES * LANES, LANES), window)

    def red_hop(k):
        t = (d + k) % replicas
        return remote(redsend.at[:, window_of(t)], redin.at[d], rs.at[k], rr.at[k], (s, t))

    for k in range(1, replicas):
        red_hop(k).start()
    redin[d] = redsend[:, window_of(d)]
    for k in range(1, replicas):
        red_hop(k).wait_recv()
    reduced = jnp.sum(redin[...].astype(jnp.float32), axis=0)
    reduced = pltpu.roll(reduced, (window - span * d % LANES) % window, axis=1)
    out_ref[: 2 * rank] = reduced

    for copy in swaps(mine):
        copy.wait_send()
    for j in range(2):

        def one(w, carry):
            k, sub = 1 + w // SUBS, w % SUBS
            for way in range(2):
                ours = (sub < SUBS // 2) if way == 0 else (sub >= SUBS // 2)

                @pl.when((k < last) | ours)
                def _(way=way):
                    sending(j, way, k, sub).wait_send()

            return carry

        lax.fori_loop(0, last * SUBS, one, 0)

    @pl.when(top)
    def _():
        def one(o, carry):
            across(o).wait_send()
            return carry

        lax.fori_loop(0, replicas, one, 0)

        def two(r, carry):
            down_hop(block_at(r)).wait_send()
            return carry

        lax.fori_loop(0, replicas - 2, two, 0)
        for i in range(2):
            for m in range(slots):
                late_hop(i, m).wait_send()

    @pl.when(second)
    def _():
        def one(r, carry):
            relay(block_at(r)).wait_send()
            return carry

        lax.fori_loop(0, replicas - 2, one, 0)
        for i in range(2):
            for m in range(slots):
                late_relay(i, m, 0).wait_send()

    @pl.when(y < sections // 2 - 1)
    def _():
        def one(w, carry):
            m, part = w // QUADS, w % QUADS
            quad_across(m, part, c).wait_send()

            @pl.when(y > 0)
            def _():
                quad_down(m, part).wait_send()

            @pl.when(y < sections // 2 - 2)
            def _():
                quad_relay(m, part, c).wait_send()

            return carry

        lax.fori_loop(0, slots * QUADS, one, 0)

    for k in range(1, sections):
        sq_hop(k).wait_send()
    for k in range(1, replicas):
        red_hop(k).wait_send()


def on_device(acts, cotangent, frozen, down_adapter, up_adapter, example_ids, lengths):
    sections = lax.axis_size("section")
    replicas = lax.axis_size("dp")
    layer_inputs = acts[0]
    slots = example_ids.shape[1]
    width, features = layer_inputs.shape
    tokens = width // slots
    rank = down_adapter.shape[1]
    clip_scale = math.sqrt(2.0 * rank * features) / math.sqrt(replicas * slots)
    span = features // replicas
    half = span // 2
    window = -(-(span + LANES - 1) // LANES) * LANES
    vmem = pl.BlockSpec(memory_space=pltpu.VMEM)
    smem = pl.BlockSpec(memory_space=pltpu.SMEM)
    hbm = pl.BlockSpec(memory_space=pl.ANY)
    dma = pltpu.SemaphoreType.DMA
    bf16, f32 = jnp.bfloat16, jnp.float32
    out = pl.pallas_call(
        functools.partial(kernel, sections, replicas, slots, clip_scale),
        out_shape=jax.ShapeDtypeStruct((2 * rank + 8, window), f32),
        in_specs=[hbm, hbm, hbm, vmem, vmem, smem, smem],
        out_specs=vmem,
        scratch_shapes=[
            pltpu.VMEM((2, replicas, half, features), bf16),
            pltpu.VMEM((2, replicas, 2, half, width), bf16),
            pltpu.VMEM((replicas, half, width), bf16),
            pltpu.VMEM((width, features), bf16),
            pltpu.VMEM((width, features), bf16),
            pltpu.VMEM((2, rank, features), bf16),
            pltpu.VMEM((2, rank, features), bf16),
            pltpu.VMEM((2, replicas, 2, half, rank), bf16),
            pltpu.VMEM((2, rank, width), bf16),
            pltpu.VMEM((rank, width), bf16),
            pltpu.VMEM((slots, 2 * rank, features), f32),
            pltpu.VMEM((8, LANES), f32),
            pltpu.VMEM((sections, 8, LANES), f32),
            pltpu.VMEM((2 * rank, features + LANES), bf16),
            pltpu.VMEM((replicas, 2 * rank, window), bf16),
            pltpu.VMEM((8, width), f32),
            dma((3,)), dma((3,)), dma((3,)),
            dma((2, 2, replicas // 2, SUBS)), dma((2, 2, replicas // 2, SUBS)),
            dma((replicas,)), dma((replicas,)),
            dma((replicas,)), dma((replicas,)),
            dma((replicas,)), dma((replicas,)),
            dma((sections,)), dma((sections,)),
            dma((replicas,)), dma((replicas,)),
            dma((2, slots)), dma((2, slots)), dma((2, slots)), dma((2, slots)),
        ],
        compiler_params=pltpu.CompilerParams(
            collective_id=0, has_side_effects=True, vmem_limit_bytes=62 * 1024 * 1024
        ),
    )(frozen[0], cotangent, layer_inputs, up_adapter[0], down_adapter[0], example_ids, lengths)
    return (out[None, :rank, :span], out[None, rank : 2 * rank, :span], out[2 * rank : 2 * rank + 1, :slots])


def solution(mesh):
    in_specs = (
        P("section", "dp", None),
        P("dp", None),
        P("section", "dp", None),
        P("section", None, None),
        P("section", None, None),
        P("dp", None),
        P("dp", None),
    )
    out_specs = (P("section", None, "dp"), P("section", None, "dp"), P("dp", None))
    return jax.shard_map(
        on_device, mesh=mesh, in_specs=in_specs, out_specs=out_specs, check_vma=False
    )
```

```python
import functools
import math

import jax
import jax.numpy as jnp
from jax import lax
from jax.experimental import pallas as pl
from jax.experimental.pallas import tpu as pltpu
from jax.sharding import PartitionSpec as P

MESH = pl.DeviceIdType.MESH
NT = (((1,), (1,)), ((), ()))
LANES = 128
SIDE = 4
SUBS = 7
AIDS = 2
QUADS = 4


def fdot(a, b, dims=None):
    if dims is None:
        return jnp.dot(a, b, preferred_element_type=jnp.float32)
    return lax.dot_general(a, b, dims, preferred_element_type=jnp.float32)


def kernel(
    sections, replicas, slots, clip_scale,
    frozen_hbm, cot_hbm, acts_hbm, up_ref, down_ref, ids_ref, lengths_ref,
    out_ref,
    wbuf, gbuf, obuf, abuf, cbuf, upb, downb, dtb, ugb, dab, tbuf, sqbuf, sqall, redsend, redin,
    live,
    local_sem, swap_send, swap_recv, ws, wr, es, er, ys, yr, fs, fr, sqs, sqr, rs, rr,
    hbuf, gs, gr, hws, hwr, hs, hr,
):
    s = lax.axis_index("section")
    d = lax.axis_index("dp")
    y, c = s // 2, s % 2
    top = y == sections // 2 - 1
    second = y == sections // 2 - 2
    half = wbuf.shape[2]
    features = wbuf.shape[3]
    width = gbuf.shape[4]
    tokens = width // slots
    rank = up_ref.shape[0]
    span = features // replicas
    window = redin.shape[2]
    cols = features // SUBS
    group = replicas // QUADS
    partner = s + 1 - 2 * c
    below = (s + sections - 2) % sections
    aids = jnp.where(y == 0, 2, jnp.where(y == 1, 1, 0))
    gifts = jnp.where(top, 2, jnp.where(second, 1, 0))
    skip = jnp.where(y == 0, SUBS, gifts)
    above = (s + 2) % sections
    gift_to = jnp.where(top, above, below)
    aid_to = jnp.where(y == 0, below, above)
    mine = 1 - c

    z, x = d // SIDE, d % SIDE
    q = (x + 1) % SIDE
    p = (1 - c) * (SIDE * z + (z + x) % SIDE) + c * (SIDE * q + (z + q + 3) % SIDE)

    def device_at(pos):
        pos = (pos + 2 * replicas) % replicas
        hi, lo = pos // SIDE, pos % SIDE
        first = SIDE * hi + (lo + SIDE - hi) % SIDE
        second = SIDE * ((lo + 1 + SIDE - hi) % SIDE) + (hi + 3) % SIDE
        return (1 - c) * first + c * second

    def remote(src, dst, send, recv, device):
        return pltpu.make_async_remote_copy(
            src_ref=src, dst_ref=dst, send_sem=send, recv_sem=recv,
            device_id=device, device_id_type=MESH,
        )

    barrier = pltpu.get_barrier_semaphore()
    for k in range(1, sections):
        pl.semaphore_signal(barrier, inc=1, device_id=((s + k) % sections, d), device_id_type=MESH)
    for k in range(1, replicas):
        pl.semaphore_signal(barrier, inc=1, device_id=(s, (d + k) % replicas), device_id_type=MESH)

    def half_rows(h):
        return frozen_hbm.at[pl.ds(pl.multiple_of(h * half, 16), half)]

    own_copy = pltpu.make_async_copy(half_rows(c), wbuf.at[mine, d], local_sem.at[0])
    acts_copy = pltpu.make_async_copy(acts_hbm, abuf, local_sem.at[1])
    cot_copy = pltpu.make_async_copy(cot_hbm, cbuf, local_sem.at[2])
    own_copy.start()
    acts_copy.start()

    @pl.when(top)
    def _():
        cot_copy.start()

    place = lax.broadcasted_iota(jnp.int32, (8, tokens), 1)
    for m in range(slots):
        length = jnp.int32(0)
        for k in range(slots):
            length = length + jnp.where(ids_ref[0, m] == k, lengths_ref[0, k], 0)
        live[:, m * tokens : (m + 1) * tokens] = jnp.where(place < length, 1.0, 0.0)
    upb[mine] = up_ref[...]
    downb[mine] = down_ref[...]
    sqbuf[...] = jnp.zeros_like(sqbuf)
    redsend[:, features:] = jnp.zeros_like(redsend[:, features:])
    pl.semaphore_wait(barrier, sections - 1 + replicas - 1)

    def swaps(j):
        to = (partner, d)
        return (
            remote(half_rows(1 - c), wbuf.at[j, d], swap_send.at[0], swap_recv.at[0], to),
            remote(up_ref, upb.at[j], swap_send.at[1], swap_recv.at[1], to),
            remote(down_ref, downb.at[j], swap_send.at[2], swap_recv.at[2], to),
        )

    for copy in swaps(mine):
        copy.start()
    own_copy.wait()

    def swapped():
        for copy in swaps(c):
            copy.wait_recv()

    def ring(j, way, k, sub, origin):
        at = wbuf.at[j, device_at(origin), :, pl.ds(pl.multiple_of(sub * cols, LANES), cols)]
        to = (s, device_at(p + 1 - 2 * way))
        return remote(at, at, ws.at[j, way, k - 1, sub], wr.at[j, way, k - 1, sub], to)

    def sending(j, way, k, sub):
        return ring(j, way, k, sub, p - (1 - 2 * way) * (k - 1))

    def arriving(j, way, k, sub):
        return ring(j, way, k, sub, p - (1 - 2 * way) * k)

    last = replicas // 2

    def ours(way, sub):
        return (sub <= SUBS // 2) if way == 0 else (sub > SUBS // 2)

    def travels(j, sub):
        return (sub >= skip) if j == 1 else (sub >= 0)

    def begin(j):
        def one(sub, carry):
            @pl.when(travels(j, sub))
            def _():
                for way in range(2):
                    sending(j, way, 1, sub).start()

            return carry

        lax.fori_loop(0, SUBS, one, 0)

    def serve(j, k, sub):
        for way in range(2):

            @pl.when(travels(j, sub) & ((k < last) | ours(way, sub)))
            def _(way=way):
                arriving(j, way, k, sub).wait_recv()

            @pl.when(travels(j, sub) & ((k < last - 1) | ((k == last - 1) & ours(way, sub))))
            def _(way=way):
                sending(j, way, k + 1, sub).start()

    def aid_cols(h):
        return pl.ds(h * cols, cols)

    def gift(h):
        src = wbuf.at[1, d, :, aid_cols(h)]
        return remote(src, hbuf.at[h, d], gs.at[h], gr.at[h], (gift_to, d))

    def lift(h, o):
        return remote(hbuf.at[h, o], wbuf.at[1, o, :, aid_cols(h)], hs.at[h, o], hr.at[h, o], (aid_to, d))

    def aid_ring(h, way, k, origin):
        at = hbuf.at[h, device_at(origin)]
        to = (s, device_at(p + 1 - 2 * way))
        return remote(at, at, hws.at[h, way, k - 1], hwr.at[h, way, k - 1], to)

    def aid_sending(h, way, k):
        return aid_ring(h, way, k, p - (1 - 2 * way) * (k - 1))

    def aid_arriving(h, way, k):
        return aid_ring(h, way, k, p - (1 - 2 * way) * k)

    def aid_begin():
        for h in range(AIDS):

            @pl.when(h < aids)
            def _(h=h):
                gift(h).wait_recv()
                for way in range(2):
                    aid_sending(h, way, 1).start()

    def aid_serve(h, k):
        for way in range(2):
            turn = way == 1 - h

            @pl.when((h < aids) & ((k < last) | turn))
            def _(way=way):
                aid_arriving(h, way, k).wait_recv()

            @pl.when((h < aids) & ((k < last - 1) | ((k == last - 1) & turn)))
            def _(way=way):
                aid_sending(h, way, k + 1).start()

            @pl.when((h < aids) & ((k < last) | turn))
            def _(way=way):
                lift(h, device_at(p - (1 - 2 * way) * k)).start()

    def steps(first, count, work=None):
        def step(i, carry):
            k = first + i

            def wave(sub, carry):
                serve(0, k, sub)
                if work is not None:
                    work(i * SUBS + sub)
                return carry

            lax.fori_loop(0, SUBS, wave, 0)
            for h in range(AIDS):
                aid_serve(h, k)
            return carry

        lax.fori_loop(0, count, step, 0)

    def waves(first, count, work):
        def wave(w, carry):
            serve(1, first + w // SUBS, w % SUBS)
            work(w)
            return carry

        lax.fori_loop(0, count * SUBS, wave, 0)

    def lanes(m):
        return pl.ds(pl.multiple_of(m * tokens, LANES), tokens)

    def seed(w):
        @pl.when(top & (w < slots * QUADS))
        def _():
            m, part = w // QUADS, w % QUADS
            wide = features // QUADS
            block = cbuf[
                pl.ds(pl.multiple_of(m * tokens, tokens), tokens),
                pl.ds(pl.multiple_of(part * wide, LANES), wide),
            ]
            turned = block.astype(jnp.float32).T * live[0:1, lanes(m)]
            gbuf[0, pl.ds(part * group, group), :, :, lanes(m)] = turned.astype(jnp.bfloat16).reshape(
                group, 2, half, tokens
            )

    @pl.when(c == 0)
    def _():
        swapped()

    begin(0)

    @pl.when(c == 1)
    def _():
        swapped()

    for h in range(AIDS):

        @pl.when(h < gifts)
        def _(h=h):
            gift(h).start()

    aid_begin()


    @pl.when(top)
    def _():
        cot_copy.wait()

    steps(1, 3, seed)
    acts_copy.wait()
    dab[...] = fdot(down_ref[...], abuf[...], NT).astype(jnp.bfloat16)
    for j in range(2):
        turned = downb[j].astype(jnp.float32).T
        dtb[j] = turned.astype(jnp.bfloat16).reshape(replicas, 2, half, rank)

    def whole(j):
        return gbuf[j].reshape(features, width)

    def part_of(j, m):
        return gbuf[j, :, :, :, lanes(m)].reshape(features, tokens)

    @pl.when(top)
    def _():
        ugb[0] = fdot(upb[0], whole(0)).astype(jnp.bfloat16)

    steps(4, 4)
    begin(1)
    steps(8, 1)

    def top_product(j, o):
        got = fdot(wbuf[j, o], whole(j)) + fdot(dtb[j, o, c], ugb[j])
        return got.astype(jnp.bfloat16)

    def across(o):
        at = gbuf.at[1, o, c]
        return remote(at, at, es.at[o], er.at[o], (partner, d))

    def across_in(o):
        at = gbuf.at[1, o, 1 - c]
        return remote(at, at, es.at[o], er.at[o], (partner, d))

    def down_hop(o):
        return remote(obuf.at[o], gbuf.at[0, o, c], ys.at[o], yr.at[o], (below, d))

    def relay(o):
        at = gbuf.at[0, o, c]
        return remote(at, at, fs.at[o], fr.at[o], (partner, d))

    def relay_in(o):
        at = gbuf.at[0, o, 1 - c]
        return remote(at, at, fs.at[o], fr.at[o], (partner, d))

    def block_at(r):
        return device_at(p - (r % 2) * ((r + 1) // 2) + (1 - r % 2) * (r // 2))

    def upper(w):
        @pl.when(top)
        def _():
            def one(o, carry):
                gbuf[1, o, c] = top_product(0, o)
                across(o).start()
                return carry

            lax.fori_loop(8 * w // SUBS, 8 * (w + 1) // SUBS, one, 0)

    def lower(r):
        o = block_at(r)

        @pl.when(r > 0)
        def _():
            for h in range(AIDS):
                lift(h, o).wait_recv()

        obuf[o] = top_product(1, o)
        down_hop(o).start()

    def hand_on(r):
        o = block_at(r)
        down_hop(o).wait_recv()
        relay(o).start()

    waves(1, 2, upper)

    @pl.when(top)
    def _():
        def one(o, carry):
            across_in(o).wait_recv()
            return carry

        lax.fori_loop(0, replicas, one, 0)
        ugb[1] = fdot(upb[1], whole(1)).astype(jnp.bfloat16)

    def middle(w):
        step, turn = w // SUBS, w % SUBS
        first = step == 0

        @pl.when(top & ((first & (turn < 5)) | ((step > 0) & ((turn == 2) | (turn == 4)))))
        def _():
            lower(jnp.where(first, turn, 3 + 2 * step + (turn - 2) // 2))

        few = jnp.where(step < 3, 4, jnp.where(step == 3, 3, 2))
        base = jnp.where(step < 4, 4 * (step - 1), 11)

        @pl.when(second & (step > 0) & (turn >= 1) & (turn <= few))
        def _():
            hand_on(base + turn - 1)

    waves(3, 5, middle)

    def final(w):
        @pl.when(top & ((w == 2) | (w == 4)))
        def _():
            lower(12 + w // 2)

        @pl.when(second & (w == 1))
        def _():
            hand_on(13)

        @pl.when(second & (w == 5))
        def _():
            hand_on(14)

    waves(8, 1, final)

    @pl.when(top)
    def _():
        lower(replicas - 1)

    @pl.when(second)
    def _():
        hand_on(replicas - 1)

        def two(o, carry):
            relay_in(o).wait_recv()
            return carry

        lax.fori_loop(0, replicas, two, 0)

        def three(r, carry):
            lift(0, block_at(r)).wait_recv()
            return carry

        lax.fori_loop(1, replicas, three, 0)

    def terms(m):
        inputs = abuf[pl.ds(pl.multiple_of(m * tokens, tokens), tokens), :]
        down_term = fdot(ugb[mine, :, lanes(m)], inputs)
        up_term = fdot(dab[:, lanes(m)], part_of(mine, m), NT)
        tbuf[m, :rank, :] = down_term
        tbuf[m, rank:, :] = up_term
        square = jnp.sum(down_term * down_term + up_term * up_term, axis=0, keepdims=True)
        square = jnp.sum(square, axis=1, keepdims=True)
        sqbuf[pl.ds(m, 1), :] = jnp.broadcast_to(square, (1, LANES))

    def quad(ref, j, m, part, side):
        return ref.at[j, pl.ds(part * group, group), side, :, lanes(m)]

    def quad_product(j, m, part):
        blocks = pl.ds(part * group, group)
        weight = wbuf[j, blocks].reshape(group * half, features)
        adapter = dtb[j, blocks, c].reshape(group * half, rank)
        got = fdot(weight, part_of(j, m)) + fdot(adapter, ugb[j, :, lanes(m)])
        return got.astype(jnp.bfloat16).reshape(group, half, tokens)

    def quad_across(m, part, side):
        at = quad(gbuf, 1, m, part, side)
        return remote(at, at, es.at[m * QUADS + part], er.at[m * QUADS + part], (partner, d))

    def quad_down(m, part):
        src = obuf.at[pl.ds(part * group, group), :, lanes(m)]
        at = m * QUADS + part
        return remote(src, quad(gbuf, 0, m, part, c), ys.at[at], yr.at[at], (below, d))

    def quad_relay(m, part, side):
        at = quad(gbuf, 0, m, part, side)
        return remote(at, at, fs.at[m * QUADS + part], fr.at[m * QUADS + part], (partner, d))

    def each_quad(work):
        def one(part, carry):
            work(part)
            return carry

        lax.fori_loop(0, QUADS, one, 0)

    def odd_whole(m):
        ugb[0, :, lanes(m)] = fdot(upb[0], part_of(0, m)).astype(jnp.bfloat16)

        def odd(part):
            gbuf[1, pl.ds(part * group, group), c, :, lanes(m)] = quad_product(0, m, part)
            quad_across(m, part, c).start()

        each_quad(odd)

    def slot(m, carry):
        @pl.when(second)
        def _():
            odd_whole(m)

        @pl.when(y < sections // 2 - 2)
        def _():
            def pass_on(part):
                quad_down(m, part).wait_recv()
                quad_relay(m, part, c).start()

            each_quad(pass_on)
            each_quad(lambda part: quad_relay(m, part, 1 - c).wait_recv())
            odd_whole(m)

        @pl.when(c == 1)
        def _():
            terms(m)

        @pl.when((c == 0) & (m > 0))
        def _():
            terms(m - 1)

        each_quad(lambda part: quad_across(m, part, 1 - c).wait_recv())
        ugb[1, :, lanes(m)] = fdot(upb[1], part_of(1, m)).astype(jnp.bfloat16)

        @pl.when(y > 0)
        def _():
            def even(part):
                obuf[pl.ds(part * group, group), :, lanes(m)] = quad_product(1, m, part)
                quad_down(m, part).start()

            each_quad(even)

        return carry

    @pl.when(y < sections // 2 - 1)
    def _():
        lax.fori_loop(0, slots, slot, 0)

        @pl.when(c == 0)
        def _():
            terms(slots - 1)

    @pl.when(top)
    def _():
        def one(m, carry):
            terms(m)
            return carry

        lax.fori_loop(0, slots, one, 0)

    def sq_hop(k):
        return remote(sqbuf, sqall.at[s], sqs.at[k], sqr.at[k], ((s + k) % sections, d))

    for k in range(1, sections):
        sq_hop(k).start()
    sqall[s] = sqbuf[...]
    for k in range(1, sections):
        sq_hop(k).wait_recv()
    norm = jnp.sqrt(jnp.sum(sqall[...], axis=0))
    lane = lax.broadcasted_iota(jnp.int32, (1, LANES), 1)
    named = jnp.zeros((1, LANES), jnp.float32)
    for m in range(slots):
        named = named + jnp.where(lane == ids_ref[0, m], norm[m : m + 1, :], 0.0)
    out_ref[2 * rank :, :LANES] = jnp.broadcast_to(named, (8, LANES))
    out_ref[2 * rank :, LANES:] = jnp.zeros((8, window - LANES), jnp.float32)
    factor = clip_scale / (norm + 0.01)
    total = factor[0:1, 0:1] * tbuf[0]
    for m in range(1, slots):
        total = total + factor[m : m + 1, 0:1] * tbuf[m]
    redsend[:, :features] = total.astype(jnp.bfloat16)

    def window_of(t):
        return pl.ds(pl.multiple_of(span * t // LANES * LANES, LANES), window)

    def red_hop(k):
        t = (d + k) % replicas
        return remote(redsend.at[:, window_of(t)], redin.at[d], rs.at[k], rr.at[k], (s, t))

    for k in range(1, replicas):
        red_hop(k).start()
    redin[d] = redsend[:, window_of(d)]
    for k in range(1, replicas):
        red_hop(k).wait_recv()
    reduced = jnp.sum(redin[...].astype(jnp.float32), axis=0)
    reduced = pltpu.roll(reduced, (window - span * d % LANES) % window, axis=1)
    out_ref[: 2 * rank] = reduced

    for copy in swaps(mine):
        copy.wait_send()
    for j in range(2):

        def one(w, carry):
            k, sub = 1 + w // SUBS, w % SUBS
            for way in range(2):

                @pl.when(travels(j, sub) & ((k < last) | ours(way, sub)))
                def _(way=way):
                    sending(j, way, k, sub).wait_send()

            return carry

        lax.fori_loop(0, last * SUBS, one, 0)

    for h in range(AIDS):

        @pl.when(h < gifts)
        def _(h=h):
            gift(h).wait_send()

        @pl.when(h < aids)
        def _(h=h):
            for way in range(2):
                for k in range(1, last + 1):
                    if k < last or way == 1 - h:
                        aid_sending(h, way, k).wait_send()

            def one(r, carry):
                lift(h, block_at(r)).wait_send()
                return carry

            lax.fori_loop(1, replicas, one, 0)

    @pl.when(top)
    def _():
        def one(o, carry):
            across(o).wait_send()
            down_hop(o).wait_send()
            return carry

        lax.fori_loop(0, replicas, one, 0)

    @pl.when(second)
    def _():
        def one(o, carry):
            relay(o).wait_send()
            return carry

        lax.fori_loop(0, replicas, one, 0)

    @pl.when(y < sections // 2 - 1)
    def _():
        def one(w, carry):
            m, part = w // QUADS, w % QUADS
            quad_across(m, part, c).wait_send()

            @pl.when(y > 0)
            def _():
                quad_down(m, part).wait_send()

            @pl.when(y < sections // 2 - 2)
            def _():
                quad_relay(m, part, c).wait_send()

            return carry

        lax.fori_loop(0, slots * QUADS, one, 0)

    for k in range(1, sections):
        sq_hop(k).wait_send()
    for k in range(1, replicas):
        red_hop(k).wait_send()


def on_device(acts, cotangent, frozen, down_adapter, up_adapter, example_ids, lengths):
    sections = lax.axis_size("section")
    replicas = lax.axis_size("dp")
    layer_inputs = acts[0]
    slots = example_ids.shape[1]
    width, features = layer_inputs.shape
    tokens = width // slots
    rank = down_adapter.shape[1]
    clip_scale = math.sqrt(2.0 * rank * features) / math.sqrt(replicas * slots)
    span = features // replicas
    half = span // 2
    window = -(-(span + LANES - 1) // LANES) * LANES
    vmem = pl.BlockSpec(memory_space=pltpu.VMEM)
    smem = pl.BlockSpec(memory_space=pltpu.SMEM)
    hbm = pl.BlockSpec(memory_space=pl.ANY)
    dma = pltpu.SemaphoreType.DMA
    bf16, f32 = jnp.bfloat16, jnp.float32
    out = pl.pallas_call(
        functools.partial(kernel, sections, replicas, slots, clip_scale),
        out_shape=jax.ShapeDtypeStruct((2 * rank + 8, window), f32),
        in_specs=[hbm, hbm, hbm, vmem, vmem, smem, smem],
        out_specs=vmem,
        scratch_shapes=[
            pltpu.VMEM((2, replicas, half, features), bf16),
            pltpu.VMEM((2, replicas, 2, half, width), bf16),
            pltpu.VMEM((replicas, half, width), bf16),
            pltpu.VMEM((width, features), bf16),
            pltpu.VMEM((width, features), bf16),
            pltpu.VMEM((2, rank, features), bf16),
            pltpu.VMEM((2, rank, features), bf16),
            pltpu.VMEM((2, replicas, 2, half, rank), bf16),
            pltpu.VMEM((2, rank, width), bf16),
            pltpu.VMEM((rank, width), bf16),
            pltpu.VMEM((slots, 2 * rank, features), f32),
            pltpu.VMEM((8, LANES), f32),
            pltpu.VMEM((sections, 8, LANES), f32),
            pltpu.VMEM((2 * rank, features + LANES), bf16),
            pltpu.VMEM((replicas, 2 * rank, window), bf16),
            pltpu.VMEM((8, width), f32),
            dma((3,)), dma((3,)), dma((3,)),
            dma((2, 2, replicas // 2, SUBS)), dma((2, 2, replicas // 2, SUBS)),
            dma((replicas,)), dma((replicas,)),
            dma((replicas,)), dma((replicas,)),
            dma((replicas,)), dma((replicas,)),
            dma((sections,)), dma((sections,)),
            dma((replicas,)), dma((replicas,)),
            pltpu.VMEM((AIDS, replicas, half, features // SUBS), bf16),
            dma((AIDS,)), dma((AIDS,)),
            dma((AIDS, 2, replicas // 2)), dma((AIDS, 2, replicas // 2)),
            dma((AIDS, replicas)), dma((AIDS, replicas)),
        ],
        compiler_params=pltpu.CompilerParams(
            collective_id=0, has_side_effects=True, vmem_limit_bytes=62 * 1024 * 1024
        ),
    )(frozen[0], cotangent, layer_inputs, up_adapter[0], down_adapter[0], example_ids, lengths)
    return (out[None, :rank, :span], out[None, rank : 2 * rank, :span], out[2 * rank : 2 * rank + 1, :slots])


def solution(mesh):
    in_specs = (
        P("section", "dp", None),
        P("dp", None),
        P("section", "dp", None),
        P("section", None, None),
        P("section", None, None),
        P("dp", None),
        P("dp", None),
    )
    out_specs = (P("section", None, "dp"), P("section", None, "dp"), P("dp", None))
    return jax.shard_map(
        on_device, mesh=mesh, in_specs=in_specs, out_specs=out_specs, check_vma=False
    )
```

```python
import functools
import math

import jax
import jax.numpy as jnp
from jax import lax
from jax.experimental import pallas as pl
from jax.experimental.pallas import tpu as pltpu
from jax.sharding import PartitionSpec as P

MESH = pl.DeviceIdType.MESH
NT = (((1,), (1,)), ((), ()))
LANES = 128
SIDE = 4
SUBS = 7
GIFTS = 2
AIDS = 4
LATE = 4
QUADS = 4


def fdot(a, b, dims=None):
    if dims is None:
        return jnp.dot(a, b, preferred_element_type=jnp.float32)
    return lax.dot_general(a, b, dims, preferred_element_type=jnp.float32)


def kernel(
    sections, replicas, slots, clip_scale,
    frozen_hbm, cot_hbm, acts_hbm, up_ref, down_ref, ids_ref, lengths_ref,
    out_ref,
    wbuf, gbuf, obuf, abuf, cbuf, upb, downb, dtb, ugb, dab, tbuf, sqbuf, sqall, redsend, redin,
    live,
    local_sem, swap_send, swap_recv, ws, wr, es, er, ys, yr, fs, fr, sqs, sqr, rs, rr,
    hbuf, gs, gr, hws, hwr, hs, hr, y2s, y2r, f2s, f2r,
):
    s = lax.axis_index("section")
    d = lax.axis_index("dp")
    y, c = s // 2, s % 2
    top = y == sections // 2 - 1
    second = y == sections // 2 - 2
    half = wbuf.shape[2]
    features = wbuf.shape[3]
    width = gbuf.shape[4]
    tokens = width // slots
    rank = up_ref.shape[0]
    span = features // replicas
    window = redin.shape[2]
    cols = features // SUBS
    group = replicas // QUADS
    partner = s + 1 - 2 * c
    below = (s + sections - 2) % sections
    aids = jnp.where(y == 0, AIDS, jnp.where(y == 1, GIFTS, 0))
    given = y > 0
    skip = jnp.where(y == 0, SUBS, GIFTS)
    above = (s + 2) % sections
    gift_to = jnp.where(top, above, below)
    gift_at = jnp.where(y == 1, GIFTS, 0)
    mine = 1 - c

    z, x = d // SIDE, d % SIDE
    q = (x + 1) % SIDE
    p = (1 - c) * (SIDE * z + (z + x) % SIDE) + c * (SIDE * q + (z + q + 3) % SIDE)

    def device_at(pos):
        pos = (pos + 2 * replicas) % replicas
        hi, lo = pos // SIDE, pos % SIDE
        first = SIDE * hi + (lo + SIDE - hi) % SIDE
        second = SIDE * ((lo + 1 + SIDE - hi) % SIDE) + (hi + 3) % SIDE
        return (1 - c) * first + c * second

    p2 = c * (SIDE * z + (z + x) % SIDE) + (1 - c) * (SIDE * q + (z + q + 3) % SIDE)

    def other_device_at(pos):
        pos = (pos + 2 * replicas) % replicas
        hi, lo = pos // SIDE, pos % SIDE
        first = SIDE * hi + (lo + SIDE - hi) % SIDE
        second = SIDE * ((lo + 1 + SIDE - hi) % SIDE) + (hi + 3) % SIDE
        return c * first + (1 - c) * second

    def remote(src, dst, send, recv, device):
        return pltpu.make_async_remote_copy(
            src_ref=src, dst_ref=dst, send_sem=send, recv_sem=recv,
            device_id=device, device_id_type=MESH,
        )

    barrier = pltpu.get_barrier_semaphore()
    for k in range(1, sections):
        pl.semaphore_signal(barrier, inc=1, device_id=((s + k) % sections, d), device_id_type=MESH)
    for k in range(1, replicas):
        pl.semaphore_signal(barrier, inc=1, device_id=(s, (d + k) % replicas), device_id_type=MESH)

    def half_rows(h):
        return frozen_hbm.at[pl.ds(pl.multiple_of(h * half, 16), half)]

    own_copy = pltpu.make_async_copy(half_rows(c), wbuf.at[mine, d], local_sem.at[0])
    acts_copy = pltpu.make_async_copy(acts_hbm, abuf, local_sem.at[1])
    cot_copy = pltpu.make_async_copy(cot_hbm, cbuf, local_sem.at[2])
    own_copy.start()
    acts_copy.start()

    @pl.when(top)
    def _():
        cot_copy.start()

    place = lax.broadcasted_iota(jnp.int32, (8, tokens), 1)
    for m in range(slots):
        length = jnp.int32(0)
        for k in range(slots):
            length = length + jnp.where(ids_ref[0, m] == k, lengths_ref[0, k], 0)
        live[:, m * tokens : (m + 1) * tokens] = jnp.where(place < length, 1.0, 0.0)
    upb[mine] = up_ref[...]
    downb[mine] = down_ref[...]
    sqbuf[...] = jnp.zeros_like(sqbuf)
    redsend[:, features:] = jnp.zeros_like(redsend[:, features:])
    pl.semaphore_wait(barrier, sections - 1 + replicas - 1)

    def swaps(j):
        to = (partner, d)
        return (
            remote(half_rows(1 - c), wbuf.at[j, d], swap_send.at[0], swap_recv.at[0], to),
            remote(up_ref, upb.at[j], swap_send.at[1], swap_recv.at[1], to),
            remote(down_ref, downb.at[j], swap_send.at[2], swap_recv.at[2], to),
        )

    for copy in swaps(mine):
        copy.start()
    own_copy.wait()

    def swapped():
        for copy in swaps(c):
            copy.wait_recv()

    def ring(j, way, k, sub, origin):
        at = wbuf.at[j, device_at(origin), :, pl.ds(pl.multiple_of(sub * cols, LANES), cols)]
        to = (s, device_at(p + 1 - 2 * way))
        return remote(at, at, ws.at[j, way, k - 1, sub], wr.at[j, way, k - 1, sub], to)

    def sending(j, way, k, sub):
        return ring(j, way, k, sub, p - (1 - 2 * way) * (k - 1))

    def arriving(j, way, k, sub):
        return ring(j, way, k, sub, p - (1 - 2 * way) * k)

    last = replicas // 2

    def ours(way, sub):
        return (sub <= SUBS // 2) if way == 0 else (sub > SUBS // 2)

    def travels(j, sub):
        return (sub >= skip) if j == 1 else (sub >= 0)

    def begin(j):
        def one(sub, carry):
            @pl.when(travels(j, sub))
            def _():
                for way in range(2):
                    sending(j, way, 1, sub).start()

            return carry

        lax.fori_loop(0, SUBS, one, 0)

    def serve(j, k, sub):
        for way in range(2):

            @pl.when(travels(j, sub) & ((k < last) | ours(way, sub)))
            def _(way=way):
                arriving(j, way, k, sub).wait_recv()

            @pl.when(travels(j, sub) & ((k < last - 1) | ((k == last - 1) & ours(way, sub))))
            def _(way=way):
                sending(j, way, k + 1, sub).start()

    def aid_cols(h):
        return pl.ds(h * cols, cols)

    def gift(i):
        src = wbuf.at[1, d, :, aid_cols(i)]
        return remote(src, hbuf.at[gift_at + i, d], gs.at[i], gr.at[gift_at + i], (gift_to, d))

    def gift_in(h):
        return remote(wbuf.at[1, d, :, aid_cols(0)], hbuf.at[h, d], gs.at[0], gr.at[h], (gift_to, d))

    def lift(h, o):
        i = h % GIFTS
        to = jnp.where((y == 0) & (h < GIFTS), below, above)
        return remote(hbuf.at[h, o], wbuf.at[1, o, :, aid_cols(i)], hs.at[h, o], hr.at[i, o], (to, d))

    def aid_ring(h, way, k, origin):
        at = hbuf.at[h, device_at(origin)]
        to = (s, device_at(p + 1 - 2 * way))
        return remote(at, at, hws.at[h, way, k - 1], hwr.at[h, way, k - 1], to)

    def aid_sending(h, way, k):
        return aid_ring(h, way, k, p - (1 - 2 * way) * (k - 1))

    def aid_arriving(h, way, k):
        return aid_ring(h, way, k, p - (1 - 2 * way) * k)

    def aid_begin():
        for h in range(AIDS):

            @pl.when(h < aids)
            def _(h=h):
                gift_in(h).wait_recv()
                for way in range(2):
                    aid_sending(h, way, 1).start()

    def aid_serve(h, k):
        for way in range(2):
            turn = way == 1 - h % 2

            @pl.when((h < aids) & ((k < last) | turn))
            def _(way=way):
                aid_arriving(h, way, k).wait_recv()

            @pl.when((h < aids) & ((k < last - 1) | ((k == last - 1) & turn)))
            def _(way=way):
                aid_sending(h, way, k + 1).start()

            @pl.when((h < aids) & ((k < last) | turn))
            def _(way=way):
                lift(h, device_at(p - (1 - 2 * way) * k)).start()

    def steps(first, count, work=None):
        def step(i, carry):
            k = first + i

            def wave(sub, carry):
                serve(0, k, sub)
                if work is not None:
                    work(i * SUBS + sub)
                return carry

            lax.fori_loop(0, SUBS, wave, 0)
            for h in range(AIDS):
                aid_serve(h, k)
            return carry

        lax.fori_loop(0, count, step, 0)

    def waves(first, count, work):
        def wave(w, carry):
            serve(1, first + w // SUBS, w % SUBS)
            work(w)
            return carry

        lax.fori_loop(0, count * SUBS, wave, 0)

    def lanes(m):
        return pl.ds(pl.multiple_of(m * tokens, LANES), tokens)

    def seed(w):
        @pl.when(top & (w < slots * QUADS))
        def _():
            m, part = w // QUADS, w % QUADS
            wide = features // QUADS
            block = cbuf[
                pl.ds(pl.multiple_of(m * tokens, tokens), tokens),
                pl.ds(pl.multiple_of(part * wide, LANES), wide),
            ]
            turned = block.astype(jnp.float32).T * live[0:1, lanes(m)]
            gbuf[0, pl.ds(part * group, group), :, :, lanes(m)] = turned.astype(jnp.bfloat16).reshape(
                group, 2, half, tokens
            )

    @pl.when(c == 0)
    def _():
        swapped()

    begin(0)

    @pl.when(c == 1)
    def _():
        swapped()

    @pl.when(given)
    def _():
        for i in range(GIFTS):
            gift(i).start()

    aid_begin()


    @pl.when(top)
    def _():
        cot_copy.wait()

    steps(1, 3, seed)
    acts_copy.wait()
    dab[...] = fdot(down_ref[...], abuf[...], NT).astype(jnp.bfloat16)
    for j in range(2):
        turned = downb[j].astype(jnp.float32).T
        dtb[j] = turned.astype(jnp.bfloat16).reshape(replicas, 2, half, rank)

    def whole(j):
        return gbuf[j].reshape(features, width)

    def part_of(j, m):
        return gbuf[j, :, :, :, lanes(m)].reshape(features, tokens)

    @pl.when(top)
    def _():
        ugb[0] = fdot(upb[0], whole(0)).astype(jnp.bfloat16)

    steps(4, 4)
    begin(1)
    steps(8, 1)

    def top_product(j, o):
        got = fdot(wbuf[j, o], whole(j)) + fdot(dtb[j, o, c], ugb[j])
        return got.astype(jnp.bfloat16)

    def across(o):
        at = gbuf.at[1, o, c]
        return remote(at, at, es.at[o], er.at[o], (partner, d))

    def across_in(o):
        at = gbuf.at[1, o, 1 - c]
        return remote(at, at, es.at[o], er.at[o], (partner, d))

    def down_hop(o):
        return remote(obuf.at[o], gbuf.at[0, o, c], ys.at[o], yr.at[o], (below, d))

    def relay(o):
        at = gbuf.at[0, o, c]
        return remote(at, at, fs.at[o], fr.at[o], (partner, d))

    def relay_in(o):
        at = gbuf.at[0, o, 1 - c]
        return remote(at, at, fs.at[o], fr.at[o], (partner, d))

    def block_at(r):
        return device_at(p - (r % 2) * ((r + 1) // 2) + (1 - r % 2) * (r // 2))

    def other_block_at(r):
        return other_device_at(p2 - (r % 2) * ((r + 1) // 2) + (1 - r % 2) * (r // 2))

    early = replicas - LATE

    def late_hop(i, m):
        o = block_at(early + i)
        dst = gbuf.at[0, o, c, :, lanes(m)]
        return remote(obuf.at[o, :, lanes(m)], dst, y2s.at[i, m], y2r.at[i, m], (below, d))

    def late_relay(i, m):
        at = gbuf.at[0, block_at(early + i), c, :, lanes(m)]
        return remote(at, at, f2s.at[i, m], f2r.at[i, m], (partner, d))

    def late_relay_in(i, m):
        at = gbuf.at[0, other_block_at(early + i), 1 - c, :, lanes(m)]
        return remote(at, at, f2s.at[i, m], f2r.at[i, m], (partner, d))

    def upper(w):
        @pl.when(top)
        def _():
            def one(o, carry):
                gbuf[1, o, c] = top_product(0, o)
                across(o).start()
                return carry

            lax.fori_loop(8 * w // SUBS, 8 * (w + 1) // SUBS, one, 0)

    def lower(r):
        o = block_at(r)

        @pl.when(r > 0)
        def _():
            for i in range(GIFTS):
                lift(i, o).wait_recv()

        obuf[o] = top_product(1, o)

        @pl.when(r < early)
        def _():
            down_hop(o).start()

        @pl.when(r >= early)
        def _():
            late_hop(r - early, 0).start()

    def hand_on(r):
        o = block_at(r)
        down_hop(o).wait_recv()
        relay(o).start()

    waves(1, 2, upper)

    @pl.when(top)
    def _():
        def one(o, carry):
            across_in(o).wait_recv()
            return carry

        lax.fori_loop(0, replicas, one, 0)
        ugb[1] = fdot(upb[1], whole(1)).astype(jnp.bfloat16)

    def middle(w):
        step, turn = w // SUBS, w % SUBS
        first = step == 0

        @pl.when(top & ((first & (turn < 5)) | ((step > 0) & ((turn == 2) | (turn == 4)))))
        def _():
            lower(jnp.where(first, turn, 3 + 2 * step + (turn - 2) // 2))

        few = jnp.where(step == 2, 3, 2)
        base = jnp.where(step == 1, 0, jnp.where(step == 2, 2, 2 * step - 1))

        @pl.when(second & (step > 0) & (turn >= 4) & (turn < 4 + few))
        def _():
            hand_on(base + turn - 4)

    waves(3, 5, middle)

    def final(w):
        @pl.when(top & ((w == 2) | (w == 4)))
        def _():
            lower(12 + w // 2)

        @pl.when(second & ((w == 4) | (w == 6)))
        def _():
            hand_on(7 + w // 2)

    waves(8, 1, final)

    @pl.when(top)
    def _():
        lower(replicas - 1)

        def one(m, carry):
            for i in range(LATE):
                late_hop(i, m).start()
            return carry

        lax.fori_loop(1, slots, one, 0)

    @pl.when(second)
    def _():
        hand_on(early - 1)

        def two(r, carry):
            relay_in(other_block_at(r)).wait_recv()
            return carry

        lax.fori_loop(0, early, two, 0)

    @pl.when(second | (y == 1))
    def _():
        def three(r, carry):
            for i in range(GIFTS):
                lift(i, block_at(r)).wait_recv()
            return carry

        lax.fori_loop(1, replicas, three, 0)

    def terms(m):
        inputs = abuf[pl.ds(pl.multiple_of(m * tokens, tokens), tokens), :]
        down_term = fdot(ugb[mine, :, lanes(m)], inputs)
        up_term = fdot(dab[:, lanes(m)], part_of(mine, m), NT)
        tbuf[m, :rank, :] = down_term
        tbuf[m, rank:, :] = up_term
        square = jnp.sum(down_term * down_term + up_term * up_term, axis=0, keepdims=True)
        square = jnp.sum(square, axis=1, keepdims=True)
        sqbuf[pl.ds(m, 1), :] = jnp.broadcast_to(square, (1, LANES))

    def quad(ref, j, m, part, side):
        return ref.at[j, pl.ds(part * group, group), side, :, lanes(m)]

    def quad_product(j, m, part):
        blocks = pl.ds(part * group, group)
        weight = wbuf[j, blocks].reshape(group * half, features)
        adapter = dtb[j, blocks, c].reshape(group * half, rank)
        got = fdot(weight, part_of(j, m)) + fdot(adapter, ugb[j, :, lanes(m)])
        return got.astype(jnp.bfloat16).reshape(group, half, tokens)

    def quad_across(m, part, side):
        at = quad(gbuf, 1, m, part, side)
        return remote(at, at, es.at[m * QUADS + part], er.at[m * QUADS + part], (partner, d))

    def quad_down(m, part):
        src = obuf.at[pl.ds(part * group, group), :, lanes(m)]
        at = m * QUADS + part
        return remote(src, quad(gbuf, 0, m, part, c), ys.at[at], yr.at[at], (below, d))

    def quad_relay(m, part, side):
        at = quad(gbuf, 0, m, part, side)
        return remote(at, at, fs.at[m * QUADS + part], fr.at[m * QUADS + part], (partner, d))

    def each_quad(work):
        def one(part, carry):
            work(part)
            return carry

        lax.fori_loop(0, QUADS, one, 0)

    def odd_whole(m):
        ugb[0, :, lanes(m)] = fdot(upb[0], part_of(0, m)).astype(jnp.bfloat16)

        def odd(part):
            gbuf[1, pl.ds(part * group, group), c, :, lanes(m)] = quad_product(0, m, part)
            quad_across(m, part, c).start()

        each_quad(odd)

    def slot(m, carry):
        @pl.when(second)
        def _():
            for i in range(LATE):
                late_hop(i, m).wait_recv()
                late_relay(i, m).start()
            for i in range(LATE):
                late_relay_in(i, m).wait_recv()
            odd_whole(m)

        @pl.when(y < sections // 2 - 2)
        def _():
            def pass_on(part):
                quad_down(m, part).wait_recv()
                quad_relay(m, part, c).start()

            each_quad(pass_on)
            each_quad(lambda part: quad_relay(m, part, 1 - c).wait_recv())
            odd_whole(m)

        @pl.when(c == 1)
        def _():
            terms(m)

        @pl.when((c == 0) & (m > 0))
        def _():
            terms(m - 1)

        each_quad(lambda part: quad_across(m, part, 1 - c).wait_recv())
        ugb[1, :, lanes(m)] = fdot(upb[1], part_of(1, m)).astype(jnp.bfloat16)

        @pl.when(y > 0)
        def _():
            def even(part):
                obuf[pl.ds(part * group, group), :, lanes(m)] = quad_product(1, m, part)
                quad_down(m, part).start()

            each_quad(even)

        return carry

    @pl.when(y < sections // 2 - 1)
    def _():
        lax.fori_loop(0, slots, slot, 0)

        @pl.when(c == 0)
        def _():
            terms(slots - 1)

    @pl.when(top)
    def _():
        def one(m, carry):
            terms(m)
            return carry

        lax.fori_loop(0, slots, one, 0)

    def sq_hop(k):
        return remote(sqbuf, sqall.at[s], sqs.at[k], sqr.at[k], ((s + k) % sections, d))

    for k in range(1, sections):
        sq_hop(k).start()
    sqall[s] = sqbuf[...]
    for k in range(1, sections):
        sq_hop(k).wait_recv()
    norm = jnp.sqrt(jnp.sum(sqall[...], axis=0))
    lane = lax.broadcasted_iota(jnp.int32, (1, LANES), 1)
    named = jnp.zeros((1, LANES), jnp.float32)
    for m in range(slots):
        named = named + jnp.where(lane == ids_ref[0, m], norm[m : m + 1, :], 0.0)
    out_ref[2 * rank :, :LANES] = jnp.broadcast_to(named, (8, LANES))
    out_ref[2 * rank :, LANES:] = jnp.zeros((8, window - LANES), jnp.float32)
    factor = clip_scale / (norm + 0.01)
    total = factor[0:1, 0:1] * tbuf[0]
    for m in range(1, slots):
        total = total + factor[m : m + 1, 0:1] * tbuf[m]
    redsend[:, :features] = total.astype(jnp.bfloat16)

    def window_of(t):
        return pl.ds(pl.multiple_of(span * t // LANES * LANES, LANES), window)

    def red_hop(k):
        t = (d + k) % replicas
        return remote(redsend.at[:, window_of(t)], redin.at[d], rs.at[k], rr.at[k], (s, t))

    for k in range(1, replicas):
        red_hop(k).start()
    redin[d] = redsend[:, window_of(d)]
    for k in range(1, replicas):
        red_hop(k).wait_recv()
    reduced = jnp.sum(redin[...].astype(jnp.float32), axis=0)
    reduced = pltpu.roll(reduced, (window - span * d % LANES) % window, axis=1)
    out_ref[: 2 * rank] = reduced

    for copy in swaps(mine):
        copy.wait_send()
    for j in range(2):

        def one(w, carry):
            k, sub = 1 + w // SUBS, w % SUBS
            for way in range(2):

                @pl.when(travels(j, sub) & ((k < last) | ours(way, sub)))
                def _(way=way):
                    sending(j, way, k, sub).wait_send()

            return carry

        lax.fori_loop(0, last * SUBS, one, 0)

    @pl.when(given)
    def _():
        for i in range(GIFTS):
            gift(i).wait_send()

    for h in range(AIDS):

        @pl.when(h < aids)
        def _(h=h):
            for way in range(2):
                for k in range(1, last + 1):
                    if k < last or way == 1 - h % 2:
                        aid_sending(h, way, k).wait_send()

            def one(r, carry):
                lift(h, block_at(r)).wait_send()
                return carry

            lax.fori_loop(1, replicas, one, 0)

    @pl.when(top)
    def _():
        def one(o, carry):
            across(o).wait_send()
            return carry

        lax.fori_loop(0, replicas, one, 0)

        def two(r, carry):
            down_hop(block_at(r)).wait_send()
            return carry

        lax.fori_loop(0, early, two, 0)

        def three(m, carry):
            for i in range(LATE):
                late_hop(i, m).wait_send()
            return carry

        lax.fori_loop(0, slots, three, 0)

    @pl.when(second)
    def _():
        def one(r, carry):
            relay(block_at(r)).wait_send()
            return carry

        lax.fori_loop(0, early, one, 0)

        def two(m, carry):
            for i in range(LATE):
                late_relay(i, m).wait_send()
            return carry

        lax.fori_loop(0, slots, two, 0)

    @pl.when(y < sections // 2 - 1)
    def _():
        def one(w, carry):
            m, part = w // QUADS, w % QUADS
            quad_across(m, part, c).wait_send()

            @pl.when(y > 0)
            def _():
                quad_down(m, part).wait_send()

            @pl.when(y < sections // 2 - 2)
            def _():
                quad_relay(m, part, c).wait_send()

            return carry

        lax.fori_loop(0, slots * QUADS, one, 0)

    for k in range(1, sections):
        sq_hop(k).wait_send()
    for k in range(1, replicas):
        red_hop(k).wait_send()


def on_device(acts, cotangent, frozen, down_adapter, up_adapter, example_ids, lengths):
    sections = lax.axis_size("section")
    replicas = lax.axis_size("dp")
    layer_inputs = acts[0]
    slots = example_ids.shape[1]
    width, features = layer_inputs.shape
    tokens = width // slots
    rank = down_adapter.shape[1]
    clip_scale = math.sqrt(2.0 * rank * features) / math.sqrt(replicas * slots)
    span = features // replicas
    half = span // 2
    window = -(-(span + LANES - 1) // LANES) * LANES
    vmem = pl.BlockSpec(memory_space=pltpu.VMEM)
    smem = pl.BlockSpec(memory_space=pltpu.SMEM)
    hbm = pl.BlockSpec(memory_space=pl.ANY)
    dma = pltpu.SemaphoreType.DMA
    bf16, f32 = jnp.bfloat16, jnp.float32
    out = pl.pallas_call(
        functools.partial(kernel, sections, replicas, slots, clip_scale),
        out_shape=jax.ShapeDtypeStruct((2 * rank + 8, window), f32),
        in_specs=[hbm, hbm, hbm, vmem, vmem, smem, smem],
        out_specs=vmem,
        scratch_shapes=[
            pltpu.VMEM((2, replicas, half, features), bf16),
            pltpu.VMEM((2, replicas, 2, half, width), bf16),
            pltpu.VMEM((replicas, half, width), bf16),
            pltpu.VMEM((width, features), bf16),
            pltpu.VMEM((width, features), bf16),
            pltpu.VMEM((2, rank, features), bf16),
            pltpu.VMEM((2, rank, features), bf16),
            pltpu.VMEM((2, replicas, 2, half, rank), bf16),
            pltpu.VMEM((2, rank, width), bf16),
            pltpu.VMEM((rank, width), bf16),
            pltpu.VMEM((slots, 2 * rank, features), f32),
            pltpu.VMEM((8, LANES), f32),
            pltpu.VMEM((sections, 8, LANES), f32),
            pltpu.VMEM((2 * rank, features + LANES), bf16),
            pltpu.VMEM((replicas, 2 * rank, window), bf16),
            pltpu.VMEM((8, width), f32),
            dma((3,)), dma((3,)), dma((3,)),
            dma((2, 2, replicas // 2, SUBS)), dma((2, 2, replicas // 2, SUBS)),
            dma((replicas,)), dma((replicas,)),
            dma((replicas,)), dma((replicas,)),
            dma((replicas,)), dma((replicas,)),
            dma((sections,)), dma((sections,)),
            dma((replicas,)), dma((replicas,)),
            pltpu.VMEM((AIDS, replicas, half, features // SUBS), bf16),
            dma((GIFTS,)), dma((AIDS,)),
            dma((AIDS, 2, replicas // 2)), dma((AIDS, 2, replicas // 2)),
            dma((AIDS, replicas)), dma((GIFTS, replicas)),
            dma((LATE, slots)), dma((LATE, slots)), dma((LATE, slots)), dma((LATE, slots)),
        ],
        compiler_params=pltpu.CompilerParams(
            collective_id=0, has_side_effects=True, vmem_limit_bytes=62 * 1024 * 1024
        ),
    )(frozen[0], cotangent, layer_inputs, up_adapter[0], down_adapter[0], example_ids, lengths)
    return (out[None, :rank, :span], out[None, rank : 2 * rank, :span], out[2 * rank : 2 * rank + 1, :slots])


def solution(mesh):
    in_specs = (
        P("section", "dp", None),
        P("dp", None),
        P("section", "dp", None),
        P("section", None, None),
        P("section", None, None),
        P("dp", None),
        P("dp", None),
    )
    out_specs = (P("section", None, "dp"), P("section", None, "dp"), P("dp", None))
    return jax.shard_map(
        on_device, mesh=mesh, in_specs=in_specs, out_specs=out_specs, check_vma=False
    )
```

```python
import functools
import math

import jax
import jax.numpy as jnp
from jax import lax
from jax.experimental import pallas as pl
from jax.experimental.pallas import tpu as pltpu
from jax.sharding import PartitionSpec as P

MESH = pl.DeviceIdType.MESH
NT = (((1,), (1,)), ((), ()))
LANES = 128
SIDE = 4
SUBS = 7
GIFTS = 2
AIDS = 4
LATE = 4
QUADS = 4


def fdot(a, b, dims=None):
    if dims is None:
        return jnp.dot(a, b, preferred_element_type=jnp.float32)
    return lax.dot_general(a, b, dims, preferred_element_type=jnp.float32)


def kernel(
    sections, replicas, slots, clip_scale,
    frozen_hbm, cot_hbm, acts_hbm, up_ref, down_ref, ids_ref, lengths_ref,
    out_ref,
    wbuf, gbuf, obuf, abuf, cbuf, upb, downb, dtb, ugb, dab, tbuf, sqbuf, sqall, redsend, redin,
    live,
    local_sem, swap_send, swap_recv, ws, wr, es, er, ys, yr, fs, fr, sqs, sqr, rs, rr,
    hbuf, gs, gr, hws, hwr, hs, hr, y2s, y2r, f2s, f2r,
):
    s = lax.axis_index("section")
    d = lax.axis_index("dp")
    y, c = s // 2, s % 2
    top = y == sections // 2 - 1
    second = y == sections // 2 - 2
    half = wbuf.shape[2]
    features = wbuf.shape[3]
    width = gbuf.shape[4]
    tokens = width // slots
    rank = up_ref.shape[0]
    span = features // replicas
    window = redin.shape[2]
    cols = features // SUBS
    group = replicas // QUADS
    partner = s + 1 - 2 * c
    below = (s + sections - 2) % sections
    aids = jnp.where(y == 0, AIDS, jnp.where(y == 1, GIFTS, 0))
    given = y > 0
    skip = jnp.where(y == 0, SUBS, GIFTS)
    above = (s + 2) % sections
    gift_to = jnp.where(top, above, below)
    gift_at = jnp.where(y == 1, GIFTS, 0)
    mine = 1 - c

    z, x = d // SIDE, d % SIDE
    q = (x + 1) % SIDE
    p = (1 - c) * (SIDE * z + (z + x) % SIDE) + c * (SIDE * q + (z + q + 3) % SIDE)

    def device_at(pos):
        pos = (pos + 2 * replicas) % replicas
        hi, lo = pos // SIDE, pos % SIDE
        first = SIDE * hi + (lo + SIDE - hi) % SIDE
        second = SIDE * ((lo + 1 + SIDE - hi) % SIDE) + (hi + 3) % SIDE
        return (1 - c) * first + c * second

    p2 = c * (SIDE * z + (z + x) % SIDE) + (1 - c) * (SIDE * q + (z + q + 3) % SIDE)

    def other_device_at(pos):
        pos = (pos + 2 * replicas) % replicas
        hi, lo = pos // SIDE, pos % SIDE
        first = SIDE * hi + (lo + SIDE - hi) % SIDE
        second = SIDE * ((lo + 1 + SIDE - hi) % SIDE) + (hi + 3) % SIDE
        return c * first + (1 - c) * second

    def remote(src, dst, send, recv, device):
        return pltpu.make_async_remote_copy(
            src_ref=src, dst_ref=dst, send_sem=send, recv_sem=recv,
            device_id=device, device_id_type=MESH,
        )

    barrier = pltpu.get_barrier_semaphore()
    for k in range(1, sections):
        pl.semaphore_signal(barrier, inc=1, device_id=((s + k) % sections, d), device_id_type=MESH)
    for k in range(1, replicas):
        pl.semaphore_signal(barrier, inc=1, device_id=(s, (d + k) % replicas), device_id_type=MESH)

    def half_rows(h):
        return frozen_hbm.at[pl.ds(pl.multiple_of(h * half, 16), half)]

    own_copy = pltpu.make_async_copy(half_rows(c), wbuf.at[mine, d], local_sem.at[0])
    acts_copy = pltpu.make_async_copy(acts_hbm, abuf, local_sem.at[1])
    cot_copy = pltpu.make_async_copy(cot_hbm, cbuf, local_sem.at[2])
    own_copy.start()
    acts_copy.start()

    @pl.when(top)
    def _():
        cot_copy.start()

    place = lax.broadcasted_iota(jnp.int32, (8, tokens), 1)
    for m in range(slots):
        length = jnp.int32(0)
        for k in range(slots):
            length = length + jnp.where(ids_ref[0, m] == k, lengths_ref[0, k], 0)
        live[:, m * tokens : (m + 1) * tokens] = jnp.where(place < length, 1.0, 0.0)
    upb[mine] = up_ref[...]
    downb[mine] = down_ref[...]
    sqbuf[...] = jnp.zeros_like(sqbuf)
    redsend[:, features:] = jnp.zeros_like(redsend[:, features:])
    pl.semaphore_wait(barrier, sections - 1 + replicas - 1)

    def swaps(j):
        to = (partner, d)
        return (
            remote(half_rows(1 - c), wbuf.at[j, d], swap_send.at[0], swap_recv.at[0], to),
            remote(up_ref, upb.at[j], swap_send.at[1], swap_recv.at[1], to),
            remote(down_ref, downb.at[j], swap_send.at[2], swap_recv.at[2], to),
        )

    for copy in swaps(mine):
        copy.start()
    own_copy.wait()

    def swapped():
        for copy in swaps(c):
            copy.wait_recv()

    def ring(j, way, k, sub, origin):
        at = wbuf.at[j, device_at(origin), :, pl.ds(pl.multiple_of(sub * cols, LANES), cols)]
        to = (s, device_at(p + 1 - 2 * way))
        return remote(at, at, ws.at[j, way, k - 1, sub], wr.at[j, way, k - 1, sub], to)

    def sending(j, way, k, sub):
        return ring(j, way, k, sub, p - (1 - 2 * way) * (k - 1))

    def arriving(j, way, k, sub):
        return ring(j, way, k, sub, p - (1 - 2 * way) * k)

    last = replicas // 2

    def ours(way, sub):
        return (sub <= SUBS // 2) if way == 0 else (sub > SUBS // 2)

    def travels(j, sub):
        return (sub >= skip) if j == 1 else (sub >= 0)

    def begin(j):
        def one(sub, carry):
            @pl.when(travels(j, sub))
            def _():
                for way in range(2):
                    sending(j, way, 1, sub).start()

            return carry

        lax.fori_loop(0, SUBS, one, 0)

    def serve(j, k, sub):
        for way in range(2):

            @pl.when(travels(j, sub) & ((k < last) | ours(way, sub)))
            def _(way=way):
                arriving(j, way, k, sub).wait_recv()

            @pl.when(travels(j, sub) & ((k < last - 1) | ((k == last - 1) & ours(way, sub))))
            def _(way=way):
                sending(j, way, k + 1, sub).start()

    def aid_cols(h):
        return pl.ds(h * cols, cols)

    def gift(i):
        src = wbuf.at[1, d, :, aid_cols(i)]
        return remote(src, hbuf.at[gift_at + i, d], gs.at[i], gr.at[gift_at + i], (gift_to, d))

    def gift_in(h):
        return remote(wbuf.at[1, d, :, aid_cols(0)], hbuf.at[h, d], gs.at[0], gr.at[h], (gift_to, d))

    def lift(h, o):
        i = h % GIFTS
        to = jnp.where((y == 0) & (h < GIFTS), below, above)
        return remote(hbuf.at[h, o], wbuf.at[1, o, :, aid_cols(i)], hs.at[h, o], hr.at[i, o], (to, d))

    def aid_ring(h, way, k, origin):
        at = hbuf.at[h, device_at(origin)]
        to = (s, device_at(p + 1 - 2 * way))
        return remote(at, at, hws.at[h, way, k - 1], hwr.at[h, way, k - 1], to)

    def aid_sending(h, way, k):
        return aid_ring(h, way, k, p - (1 - 2 * way) * (k - 1))

    def aid_arriving(h, way, k):
        return aid_ring(h, way, k, p - (1 - 2 * way) * k)

    def aid_begin():
        for h in range(AIDS):

            @pl.when(h < aids)
            def _(h=h):
                gift_in(h).wait_recv()
                for way in range(2):
                    aid_sending(h, way, 1).start()

    def aid_serve(h, k):
        for way in range(2):
            turn = way == 1 - h % 2

            @pl.when((h < aids) & ((k < last) | turn))
            def _(way=way):
                aid_arriving(h, way, k).wait_recv()

            @pl.when((h < aids) & ((k < last - 1) | ((k == last - 1) & turn)))
            def _(way=way):
                aid_sending(h, way, k + 1).start()

            @pl.when((h < aids) & ((k < last) | turn))
            def _(way=way):
                lift(h, device_at(p - (1 - 2 * way) * k)).start()

    def steps(first, count, work=None):
        def step(i, carry):
            k = first + i

            def wave(sub, carry):
                serve(0, k, sub)
                if work is not None:
                    work(i * SUBS + sub)
                return carry

            lax.fori_loop(0, SUBS, wave, 0)
            for h in range(AIDS):
                aid_serve(h, k)
            return carry

        lax.fori_loop(0, count, step, 0)

    def waves(first, count, work):
        def wave(w, carry):
            serve(1, first + w // SUBS, w % SUBS)
            work(w)
            return carry

        lax.fori_loop(0, count * SUBS, wave, 0)

    def lanes(m):
        return pl.ds(pl.multiple_of(m * tokens, LANES), tokens)

    def seed(w):
        @pl.when(top & (w < slots * QUADS))
        def _():
            m, part = w // QUADS, w % QUADS
            wide = features // QUADS
            block = cbuf[
                pl.ds(pl.multiple_of(m * tokens, tokens), tokens),
                pl.ds(pl.multiple_of(part * wide, LANES), wide),
            ]
            turned = block.astype(jnp.float32).T * live[0:1, lanes(m)]
            gbuf[0, pl.ds(part * group, group), :, :, lanes(m)] = turned.astype(jnp.bfloat16).reshape(
                group, 2, half, tokens
            )

    @pl.when(c == 0)
    def _():
        swapped()

    begin(0)

    @pl.when(c == 1)
    def _():
        swapped()

    @pl.when(given)
    def _():
        for i in range(GIFTS):
            gift(i).start()

    aid_begin()


    @pl.when(top)
    def _():
        cot_copy.wait()

    steps(1, 3, seed)
    acts_copy.wait()
    dab[...] = fdot(down_ref[...], abuf[...], NT).astype(jnp.bfloat16)
    for j in range(2):
        turned = downb[j].astype(jnp.float32).T
        dtb[j] = turned.astype(jnp.bfloat16).reshape(replicas, 2, half, rank)

    def whole(j):
        return gbuf[j].reshape(features, width)

    def part_of(j, m):
        return gbuf[j, :, :, :, lanes(m)].reshape(features, tokens)

    @pl.when(top)
    def _():
        ugb[0] = fdot(upb[0], whole(0)).astype(jnp.bfloat16)

    steps(4, 4)
    begin(1)
    steps(8, 1)

    def top_product(j, o):
        got = fdot(wbuf[j, o], whole(j)) + fdot(dtb[j, o, c], ugb[j])
        return got.astype(jnp.bfloat16)

    def across(o):
        at = gbuf.at[1, o, c]
        return remote(at, at, es.at[o], er.at[o], (partner, d))

    def across_in(o):
        at = gbuf.at[1, o, 1 - c]
        return remote(at, at, es.at[o], er.at[o], (partner, d))

    def down_hop(o):
        return remote(obuf.at[o], gbuf.at[0, o, c], ys.at[o], yr.at[o], (below, d))

    def relay(o):
        at = gbuf.at[0, o, c]
        return remote(at, at, fs.at[o], fr.at[o], (partner, d))

    def relay_in(o):
        at = gbuf.at[0, o, 1 - c]
        return remote(at, at, fs.at[o], fr.at[o], (partner, d))

    def block_at(r):
        return device_at(p - (r % 2) * ((r + 1) // 2) + (1 - r % 2) * (r // 2))

    def other_block_at(r):
        return other_device_at(p2 - (r % 2) * ((r + 1) // 2) + (1 - r % 2) * (r // 2))

    early = replicas - LATE

    def late_hop(i, m):
        o = block_at(early + i)
        dst = gbuf.at[0, o, c, :, lanes(m)]
        return remote(obuf.at[o, :, lanes(m)], dst, y2s.at[i, m], y2r.at[i, m], (below, d))

    def late_relay(i, m):
        at = gbuf.at[0, block_at(early + i), c, :, lanes(m)]
        return remote(at, at, f2s.at[i, m], f2r.at[i, m], (partner, d))

    def late_relay_in(i, m):
        at = gbuf.at[0, other_block_at(early + i), 1 - c, :, lanes(m)]
        return remote(at, at, f2s.at[i, m], f2r.at[i, m], (partner, d))

    def upper(w):
        @pl.when(top)
        def _():
            def one(o, carry):
                gbuf[1, o, c] = top_product(0, o)
                across(o).start()
                return carry

            lax.fori_loop(8 * w // SUBS, 8 * (w + 1) // SUBS, one, 0)

    def lower(r):
        o = block_at(r)

        @pl.when(r > 0)
        def _():
            for i in range(GIFTS):
                lift(i, o).wait_recv()

        obuf[o] = top_product(1, o)

        @pl.when(r < early)
        def _():
            down_hop(o).start()

        @pl.when(r >= early)
        def _():
            late_hop(r - early, 0).start()

    def hand_on(r):
        o = block_at(r)
        down_hop(o).wait_recv()
        relay(o).start()

    waves(1, 2, upper)

    @pl.when(top)
    def _():
        def one(o, carry):
            across_in(o).wait_recv()
            return carry

        lax.fori_loop(0, replicas, one, 0)
        ugb[1] = fdot(upb[1], whole(1)).astype(jnp.bfloat16)

    def middle(w):
        step, turn = w // SUBS, w % SUBS
        first = step == 0

        @pl.when(top & ((first & (turn < 5)) | ((step > 0) & ((turn == 2) | (turn == 4)))))
        def _():
            lower(jnp.where(first, turn, 3 + 2 * step + (turn - 2) // 2))

        few = jnp.where(step == 2, 3, 2)
        base = jnp.where(step == 1, 0, jnp.where(step == 2, 2, 2 * step - 1))

        @pl.when(second & (step > 0) & (turn >= 4) & (turn < 4 + few))
        def _():
            hand_on(base + turn - 4)

    waves(3, 5, middle)

    def final(w):
        @pl.when(top & ((w == 2) | (w == 4)))
        def _():
            lower(12 + w // 2)

        @pl.when(second & ((w == 4) | (w == 6)))
        def _():
            hand_on(7 + w // 2)

    waves(8, 1, final)

    @pl.when(top)
    def _():
        lower(replicas - 1)

        def one(m, carry):
            for i in range(LATE):
                late_hop(i, m).start()
            return carry

        lax.fori_loop(1, slots, one, 0)

    @pl.when(second)
    def _():
        hand_on(early - 1)

        def two(r, carry):
            relay_in(other_block_at(r)).wait_recv()
            return carry

        lax.fori_loop(0, early, two, 0)

    @pl.when(second | (y == 1))
    def _():
        def three(r, carry):
            for i in range(GIFTS):
                lift(i, block_at(r)).wait_recv()
            return carry

        lax.fori_loop(1, replicas, three, 0)

    def terms(m):
        inputs = abuf[pl.ds(pl.multiple_of(m * tokens, tokens), tokens), :]
        down_term = fdot(ugb[mine, :, lanes(m)], inputs)
        up_term = fdot(dab[:, lanes(m)], part_of(mine, m), NT)
        tbuf[m, :rank, :] = down_term
        tbuf[m, rank:, :] = up_term
        square = jnp.sum(down_term * down_term + up_term * up_term, axis=0, keepdims=True)
        square = jnp.sum(square, axis=1, keepdims=True)
        sqbuf[pl.ds(m, 1), :] = jnp.broadcast_to(square, (1, LANES))

    def quad(ref, j, m, part, side):
        return ref.at[j, pl.ds(part * group, group), side, :, lanes(m)]

    def quad_product(j, m, part):
        blocks = pl.ds(part * group, group)
        weight = wbuf[j, blocks].reshape(group * half, features)
        adapter = dtb[j, blocks, c].reshape(group * half, rank)
        got = fdot(weight, part_of(j, m)) + fdot(adapter, ugb[j, :, lanes(m)])
        return got.astype(jnp.bfloat16).reshape(group, half, tokens)

    def quad_across(m, part, side):
        at = quad(gbuf, 1, m, part, side)
        return remote(at, at, es.at[m * QUADS + part], er.at[m * QUADS + part], (partner, d))

    def quad_down(m, part):
        src = obuf.at[pl.ds(part * group, group), :, lanes(m)]
        at = m * QUADS + part
        return remote(src, quad(gbuf, 0, m, part, c), ys.at[at], yr.at[at], (below, d))

    def quad_relay(m, part, side):
        at = quad(gbuf, 0, m, part, side)
        return remote(at, at, fs.at[m * QUADS + part], fr.at[m * QUADS + part], (partner, d))

    def each_quad(work):
        def one(part, carry):
            work(part)
            return carry

        lax.fori_loop(0, QUADS, one, 0)

    def odd_whole(m):
        ugb[0, :, lanes(m)] = fdot(upb[0], part_of(0, m)).astype(jnp.bfloat16)

        def odd(part):
            gbuf[1, pl.ds(part * group, group), c, :, lanes(m)] = quad_product(0, m, part)
            quad_across(m, part, c).start()

        each_quad(odd)

    def slot(m, carry):
        @pl.when(second)
        def _():
            for i in range(LATE):
                late_hop(i, m).wait_recv()
                late_relay(i, m).start()
            for i in range(LATE):
                late_relay_in(i, m).wait_recv()
            odd_whole(m)

        @pl.when(y < sections // 2 - 2)
        def _():
            def pass_on(part):
                quad_down(m, part).wait_recv()
                quad_relay(m, part, c).start()

            each_quad(pass_on)
            each_quad(lambda part: quad_relay(m, part, 1 - c).wait_recv())
            odd_whole(m)

        @pl.when(c == 1)
        def _():
            terms(m)

        @pl.when((c == 0) & (m > 0))
        def _():
            terms(m - 1)

        each_quad(lambda part: quad_across(m, part, 1 - c).wait_recv())
        ugb[1, :, lanes(m)] = fdot(upb[1], part_of(1, m)).astype(jnp.bfloat16)

        @pl.when(y > 0)
        def _():
            def even(part):
                obuf[pl.ds(part * group, group), :, lanes(m)] = quad_product(1, m, part)
                quad_down(m, part).start()

            each_quad(even)

        return carry

    def drain_rings():
        for copy in swaps(mine):
            copy.wait_send()
        for j in range(2):

            def one(w, carry):
                k, sub = 1 + w // SUBS, w % SUBS
                for way in range(2):

                    @pl.when(travels(j, sub) & ((k < last) | ours(way, sub)))
                    def _(way=way):
                        sending(j, way, k, sub).wait_send()

                return carry

            lax.fori_loop(0, last * SUBS, one, 0)

        @pl.when(given)
        def _():
            for i in range(GIFTS):
                gift(i).wait_send()

        for h in range(AIDS):

            @pl.when(h < aids)
            def _(h=h):
                for way in range(2):
                    for k in range(1, last + 1):
                        if k < last or way == 1 - h % 2:
                            aid_sending(h, way, k).wait_send()

                def one(r, carry):
                    lift(h, block_at(r)).wait_send()
                    return carry

                lax.fori_loop(1, replicas, one, 0)

    pl.when(y == 0)(drain_rings)

    @pl.when(y < sections // 2 - 1)
    def _():
        lax.fori_loop(0, slots, slot, 0)

        @pl.when(c == 0)
        def _():
            terms(slots - 1)

    @pl.when(top)
    def _():
        def one(m, carry):
            terms(m)
            return carry

        lax.fori_loop(0, slots, one, 0)

    def sq_hop(k):
        return remote(sqbuf, sqall.at[s], sqs.at[k], sqr.at[k], ((s + k) % sections, d))

    for k in range(1, sections):
        sq_hop(k).start()
    sqall[s] = sqbuf[...]
    pl.when(y > 0)(drain_rings)

    @pl.when(top)
    def _():
        def one(o, carry):
            across(o).wait_send()
            return carry

        lax.fori_loop(0, replicas, one, 0)

        def two(r, carry):
            down_hop(block_at(r)).wait_send()
            return carry

        lax.fori_loop(0, early, two, 0)

        def three(m, carry):
            for i in range(LATE):
                late_hop(i, m).wait_send()
            return carry

        lax.fori_loop(0, slots, three, 0)

    @pl.when(second)
    def _():
        def one(r, carry):
            relay(block_at(r)).wait_send()
            return carry

        lax.fori_loop(0, early, one, 0)

        def two(m, carry):
            for i in range(LATE):
                late_relay(i, m).wait_send()
            return carry

        lax.fori_loop(0, slots, two, 0)

    @pl.when(y < sections // 2 - 1)
    def _():
        def one(w, carry):
            m, part = w // QUADS, w % QUADS
            quad_across(m, part, c).wait_send()

            @pl.when(y > 0)
            def _():
                quad_down(m, part).wait_send()

            @pl.when(y < sections // 2 - 2)
            def _():
                quad_relay(m, part, c).wait_send()

            return carry

        lax.fori_loop(0, slots * QUADS, one, 0)

    for k in range(1, sections):
        sq_hop(k).wait_recv()
    norm = jnp.sqrt(jnp.sum(sqall[...], axis=0))
    lane = lax.broadcasted_iota(jnp.int32, (1, LANES), 1)
    named = jnp.zeros((1, LANES), jnp.float32)
    for m in range(slots):
        named = named + jnp.where(lane == ids_ref[0, m], norm[m : m + 1, :], 0.0)
    out_ref[2 * rank :, :LANES] = jnp.broadcast_to(named, (8, LANES))
    out_ref[2 * rank :, LANES:] = jnp.zeros((8, window - LANES), jnp.float32)
    factor = clip_scale / (norm + 0.01)
    total = factor[0:1, 0:1] * tbuf[0]
    for m in range(1, slots):
        total = total + factor[m : m + 1, 0:1] * tbuf[m]
    redsend[:, :features] = total.astype(jnp.bfloat16)

    def window_of(t):
        return pl.ds(pl.multiple_of(span * t // LANES * LANES, LANES), window)

    def red_hop(k):
        t = (d + k) % replicas
        return remote(redsend.at[:, window_of(t)], redin.at[d], rs.at[k], rr.at[k], (s, t))

    for k in range(1, replicas):
        red_hop(k).start()
    redin[d] = redsend[:, window_of(d)]
    for k in range(1, replicas):
        red_hop(k).wait_recv()
    reduced = jnp.sum(redin[...].astype(jnp.float32), axis=0)
    reduced = pltpu.roll(reduced, (window - span * d % LANES) % window, axis=1)
    out_ref[: 2 * rank] = reduced

    for k in range(1, sections):
        sq_hop(k).wait_send()
    for k in range(1, replicas):
        red_hop(k).wait_send()


def on_device(acts, cotangent, frozen, down_adapter, up_adapter, example_ids, lengths):
    sections = lax.axis_size("section")
    replicas = lax.axis_size("dp")
    layer_inputs = acts[0]
    slots = example_ids.shape[1]
    width, features = layer_inputs.shape
    tokens = width // slots
    rank = down_adapter.shape[1]
    clip_scale = math.sqrt(2.0 * rank * features) / math.sqrt(replicas * slots)
    span = features // replicas
    half = span // 2
    window = -(-(span + LANES - 1) // LANES) * LANES
    vmem = pl.BlockSpec(memory_space=pltpu.VMEM)
    smem = pl.BlockSpec(memory_space=pltpu.SMEM)
    hbm = pl.BlockSpec(memory_space=pl.ANY)
    dma = pltpu.SemaphoreType.DMA
    bf16, f32 = jnp.bfloat16, jnp.float32
    out = pl.pallas_call(
        functools.partial(kernel, sections, replicas, slots, clip_scale),
        out_shape=jax.ShapeDtypeStruct((2 * rank + 8, window), f32),
        in_specs=[hbm, hbm, hbm, vmem, vmem, smem, smem],
        out_specs=vmem,
        scratch_shapes=[
            pltpu.VMEM((2, replicas, half, features), bf16),
            pltpu.VMEM((2, replicas, 2, half, width), bf16),
            pltpu.VMEM((replicas, half, width), bf16),
            pltpu.VMEM((width, features), bf16),
            pltpu.VMEM((width, features), bf16),
            pltpu.VMEM((2, rank, features), bf16),
            pltpu.VMEM((2, rank, features), bf16),
            pltpu.VMEM((2, replicas, 2, half, rank), bf16),
            pltpu.VMEM((2, rank, width), bf16),
            pltpu.VMEM((rank, width), bf16),
            pltpu.VMEM((slots, 2 * rank, features), f32),
            pltpu.VMEM((8, LANES), f32),
            pltpu.VMEM((sections, 8, LANES), f32),
            pltpu.VMEM((2 * rank, features + LANES), bf16),
            pltpu.VMEM((replicas, 2 * rank, window), bf16),
            pltpu.VMEM((8, width), f32),
            dma((3,)), dma((3,)), dma((3,)),
            dma((2, 2, replicas // 2, SUBS)), dma((2, 2, replicas // 2, SUBS)),
            dma((replicas,)), dma((replicas,)),
            dma((replicas,)), dma((replicas,)),
            dma((replicas,)), dma((replicas,)),
            dma((sections,)), dma((sections,)),
            dma((replicas,)), dma((replicas,)),
            pltpu.VMEM((AIDS, replicas, half, features // SUBS), bf16),
            dma((GIFTS,)), dma((AIDS,)),
            dma((AIDS, 2, replicas // 2)), dma((AIDS, 2, replicas // 2)),
            dma((AIDS, replicas)), dma((GIFTS, replicas)),
            dma((LATE, slots)), dma((LATE, slots)), dma((LATE, slots)), dma((LATE, slots)),
        ],
        compiler_params=pltpu.CompilerParams(
            collective_id=0, has_side_effects=True, vmem_limit_bytes=62 * 1024 * 1024
        ),
    )(frozen[0], cotangent, layer_inputs, up_adapter[0], down_adapter[0], example_ids, lengths)
    return (out[None, :rank, :span], out[None, rank : 2 * rank, :span], out[2 * rank : 2 * rank + 1, :slots])


def solution(mesh):
    in_specs = (
        P("section", "dp", None),
        P("dp", None),
        P("section", "dp", None),
        P("section", None, None),
        P("section", None, None),
        P("dp", None),
        P("dp", None),
    )
    out_specs = (P("section", None, "dp"), P("section", None, "dp"), P("dp", None))
    return jax.shard_map(
        on_device, mesh=mesh, in_specs=in_specs, out_specs=out_specs, check_vma=False
    )
```

```python
import functools
import math

import jax
import jax.numpy as jnp
from jax import lax
from jax.experimental import pallas as pl
from jax.experimental.pallas import tpu as pltpu
from jax.sharding import PartitionSpec as P

MESH = pl.DeviceIdType.MESH
NT = (((1,), (1,)), ((), ()))
LANES = 128
SIDE = 4
SUBS = 7
GIFTS = 2
AIDS = 4
LATE = 4
QUADS = 4


def fdot(a, b, dims=None):
    if dims is None:
        return jnp.dot(a, b, preferred_element_type=jnp.float32)
    return lax.dot_general(a, b, dims, preferred_element_type=jnp.float32)


def kernel(
    sections, replicas, slots, clip_scale,
    frozen_hbm, cot_hbm, acts_hbm, up_ref, down_ref, ids_ref, lengths_ref,
    out_ref,
    wbuf, gbuf, obuf, abuf, cbuf, upb, downb, dtb, ugb, dab, tbuf, sqbuf, sqall, redsend, redin,
    live,
    local_sem, swap_send, swap_recv, ws, wr, es, er, ys, yr, fs, fr, sqs, sqr, rs, rr,
    hbuf, gs, gr, hws, hwr, hs, hr, y2s, y2r, f2s, f2r,
):
    s = lax.axis_index("section")
    d = lax.axis_index("dp")
    y, c = s // 2, s % 2
    top = y == sections // 2 - 1
    second = y == sections // 2 - 2
    half = wbuf.shape[2]
    features = wbuf.shape[3]
    width = gbuf.shape[4]
    tokens = width // slots
    rank = up_ref.shape[0]
    span = features // replicas
    window = redin.shape[2]
    cols = features // SUBS
    group = replicas // QUADS
    partner = s + 1 - 2 * c
    below = (s + sections - 2) % sections
    aids = jnp.where(y == 0, AIDS, jnp.where(y == 1, GIFTS, 0))
    given = y > 0
    skip = jnp.where(y == 0, SUBS, GIFTS)
    above = (s + 2) % sections
    gift_to = jnp.where(top, above, below)
    gift_at = jnp.where(y == 1, GIFTS, 0)
    mine = 1 - c

    z, x = d // SIDE, d % SIDE
    q = (x + 1) % SIDE
    p = (1 - c) * (SIDE * z + (z + x) % SIDE) + c * (SIDE * q + (z + q + 3) % SIDE)

    def device_at(pos):
        pos = (pos + 2 * replicas) % replicas
        hi, lo = pos // SIDE, pos % SIDE
        first = SIDE * hi + (lo + SIDE - hi) % SIDE
        second = SIDE * ((lo + 1 + SIDE - hi) % SIDE) + (hi + 3) % SIDE
        return (1 - c) * first + c * second

    p2 = c * (SIDE * z + (z + x) % SIDE) + (1 - c) * (SIDE * q + (z + q + 3) % SIDE)

    def other_device_at(pos):
        pos = (pos + 2 * replicas) % replicas
        hi, lo = pos // SIDE, pos % SIDE
        first = SIDE * hi + (lo + SIDE - hi) % SIDE
        second = SIDE * ((lo + 1 + SIDE - hi) % SIDE) + (hi + 3) % SIDE
        return c * first + (1 - c) * second

    def remote(src, dst, send, recv, device):
        return pltpu.make_async_remote_copy(
            src_ref=src, dst_ref=dst, send_sem=send, recv_sem=recv,
            device_id=device, device_id_type=MESH,
        )

    barrier = pltpu.get_barrier_semaphore()
    for k in range(1, sections):
        pl.semaphore_signal(barrier, inc=1, device_id=((s + k) % sections, d), device_id_type=MESH)
    for k in range(1, replicas):
        pl.semaphore_signal(barrier, inc=1, device_id=(s, (d + k) % replicas), device_id_type=MESH)

    def half_rows(h):
        return frozen_hbm.at[pl.ds(pl.multiple_of(h * half, 16), half)]

    own_copy = pltpu.make_async_copy(half_rows(c), wbuf.at[mine, d], local_sem.at[0])
    acts_copy = pltpu.make_async_copy(acts_hbm, abuf, local_sem.at[1])
    cot_copy = pltpu.make_async_copy(cot_hbm, cbuf, local_sem.at[2])
    own_copy.start()
    acts_copy.start()

    @pl.when(top)
    def _():
        cot_copy.start()

    place = lax.broadcasted_iota(jnp.int32, (8, tokens), 1)
    for m in range(slots):
        length = jnp.int32(0)
        for k in range(slots):
            length = length + jnp.where(ids_ref[0, m] == k, lengths_ref[0, k], 0)
        live[:, m * tokens : (m + 1) * tokens] = jnp.where(place < length, 1.0, 0.0)
    upb[mine] = up_ref[...]
    downb[mine] = down_ref[...]
    sqbuf[...] = jnp.zeros_like(sqbuf)
    redsend[:, features:] = jnp.zeros_like(redsend[:, features:])
    pl.semaphore_wait(barrier, sections - 1 + replicas - 1)

    def swaps(j):
        to = (partner, d)
        return (
            remote(half_rows(1 - c), wbuf.at[j, d], swap_send.at[0], swap_recv.at[0], to),
            remote(up_ref, upb.at[j], swap_send.at[1], swap_recv.at[1], to),
            remote(down_ref, downb.at[j], swap_send.at[2], swap_recv.at[2], to),
        )

    for copy in swaps(mine):
        copy.start()
    own_copy.wait()

    def swapped():
        for copy in swaps(c):
            copy.wait_recv()

    def ring(j, way, k, sub, origin):
        at = wbuf.at[j, device_at(origin), :, pl.ds(pl.multiple_of(sub * cols, LANES), cols)]
        to = (s, device_at(p + 1 - 2 * way))
        return remote(at, at, ws.at[j, way, k - 1, sub], wr.at[j, way, k - 1, sub], to)

    def sending(j, way, k, sub):
        return ring(j, way, k, sub, p - (1 - 2 * way) * (k - 1))

    def arriving(j, way, k, sub):
        return ring(j, way, k, sub, p - (1 - 2 * way) * k)

    last = replicas // 2

    def ours(way, sub):
        return (sub <= SUBS // 2) if way == 0 else (sub > SUBS // 2)

    def travels(j, sub):
        return (sub >= skip) if j == 1 else (sub >= 0)

    def begin(j):
        def one(sub, carry):
            @pl.when(travels(j, sub))
            def _():
                for way in range(2):
                    sending(j, way, 1, sub).start()

            return carry

        lax.fori_loop(0, SUBS, one, 0)

    def serve(j, k, sub):
        for way in range(2):

            @pl.when(travels(j, sub) & ((k < last) | ours(way, sub)))
            def _(way=way):
                arriving(j, way, k, sub).wait_recv()

            @pl.when(travels(j, sub) & ((k < last - 1) | ((k == last - 1) & ours(way, sub))))
            def _(way=way):
                sending(j, way, k + 1, sub).start()

    def aid_cols(h):
        return pl.ds(h * cols, cols)

    def gift(i):
        src = wbuf.at[1, d, :, aid_cols(i)]
        return remote(src, hbuf.at[gift_at + i, d], gs.at[i], gr.at[gift_at + i], (gift_to, d))

    def gift_in(h):
        return remote(wbuf.at[1, d, :, aid_cols(0)], hbuf.at[h, d], gs.at[0], gr.at[h], (gift_to, d))

    def lift(h, o):
        i = h % GIFTS
        to = jnp.where((y == 0) & (h < GIFTS), below, above)
        return remote(hbuf.at[h, o], wbuf.at[1, o, :, aid_cols(i)], hs.at[h, o], hr.at[i, o], (to, d))

    def aid_ring(h, way, k, origin):
        at = hbuf.at[h, device_at(origin)]
        to = (s, device_at(p + 1 - 2 * way))
        return remote(at, at, hws.at[h, way, k - 1], hwr.at[h, way, k - 1], to)

    def aid_sending(h, way, k):
        return aid_ring(h, way, k, p - (1 - 2 * way) * (k - 1))

    def aid_arriving(h, way, k):
        return aid_ring(h, way, k, p - (1 - 2 * way) * k)

    def aid_begin():
        for h in range(AIDS):

            @pl.when(h < aids)
            def _(h=h):
                gift_in(h).wait_recv()
                for way in range(2):
                    aid_sending(h, way, 1).start()

    def aid_serve(h, k):
        for way in range(2):
            turn = way == 1 - h % 2

            @pl.when((h < aids) & ((k < last) | turn))
            def _(way=way):
                aid_arriving(h, way, k).wait_recv()

            @pl.when((h < aids) & ((k < last - 1) | ((k == last - 1) & turn)))
            def _(way=way):
                aid_sending(h, way, k + 1).start()

            @pl.when((h < aids) & ((k < last) | turn))
            def _(way=way):
                lift(h, device_at(p - (1 - 2 * way) * k)).start()

    def steps(first, count, work=None):
        def step(i, carry):
            k = first + i

            def wave(sub, carry):
                serve(0, k, sub)
                if work is not None:
                    work(i * SUBS + sub)
                return carry

            lax.fori_loop(0, SUBS, wave, 0)
            for h in range(AIDS):
                aid_serve(h, k)
            return carry

        lax.fori_loop(0, count, step, 0)

    def waves(first, count, work):
        def wave(w, carry):
            serve(1, first + w // SUBS, w % SUBS)
            work(w)
            return carry

        lax.fori_loop(0, count * SUBS, wave, 0)

    def lanes(m):
        return pl.ds(pl.multiple_of(m * tokens, LANES), tokens)

    def seed(w):
        @pl.when(top & (w < slots * QUADS))
        def _():
            m, part = w // QUADS, w % QUADS
            wide = features // QUADS
            block = cbuf[
                pl.ds(pl.multiple_of(m * tokens, tokens), tokens),
                pl.ds(pl.multiple_of(part * wide, LANES), wide),
            ]
            turned = block.astype(jnp.float32).T * live[0:1, lanes(m)]
            gbuf[0, pl.ds(part * group, group), :, :, lanes(m)] = turned.astype(jnp.bfloat16).reshape(
                group, 2, half, tokens
            )

    @pl.when(c == 0)
    def _():
        swapped()

    begin(0)

    @pl.when(c == 1)
    def _():
        swapped()

    @pl.when(given)
    def _():
        for i in range(GIFTS):
            gift(i).start()

    aid_begin()


    @pl.when(top)
    def _():
        cot_copy.wait()

    steps(1, 3, seed)
    acts_copy.wait()
    dab[...] = fdot(down_ref[...], abuf[...], NT).astype(jnp.bfloat16)
    for j in range(2):
        turned = downb[j].astype(jnp.float32).T
        dtb[j] = turned.astype(jnp.bfloat16).reshape(replicas, 2, half, rank)

    def whole(j):
        return gbuf[j].reshape(features, width)

    def part_of(j, m):
        return gbuf[j, :, :, :, lanes(m)].reshape(features, tokens)

    @pl.when(top)
    def _():
        ugb[0] = fdot(upb[0], whole(0)).astype(jnp.bfloat16)

    steps(4, 4)
    begin(1)
    steps(8, 1)

    def top_product(j, o):
        got = fdot(wbuf[j, o], whole(j)) + fdot(dtb[j, o, c], ugb[j])
        return got.astype(jnp.bfloat16)

    def across(o):
        at = gbuf.at[1, o, c]
        return remote(at, at, es.at[o], er.at[o], (partner, d))

    def across_in(o):
        at = gbuf.at[1, o, 1 - c]
        return remote(at, at, es.at[o], er.at[o], (partner, d))

    def down_hop(o):
        return remote(obuf.at[o], gbuf.at[0, o, c], ys.at[o], yr.at[o], (below, d))

    def relay(o):
        at = gbuf.at[0, o, c]
        return remote(at, at, fs.at[o], fr.at[o], (partner, d))

    def relay_in(o):
        at = gbuf.at[0, o, 1 - c]
        return remote(at, at, fs.at[o], fr.at[o], (partner, d))

    def block_at(r):
        return device_at(p - (r % 2) * ((r + 1) // 2) + (1 - r % 2) * (r // 2))

    def other_block_at(r):
        return other_device_at(p2 - (r % 2) * ((r + 1) // 2) + (1 - r % 2) * (r // 2))

    early = replicas - LATE

    def late_hop(i, m):
        o = block_at(early + i)
        dst = gbuf.at[0, o, c, :, lanes(m)]
        return remote(obuf.at[o, :, lanes(m)], dst, y2s.at[i, m], y2r.at[i, m], (below, d))

    def late_relay(i, m):
        at = gbuf.at[0, block_at(early + i), c, :, lanes(m)]
        return remote(at, at, f2s.at[i, m], f2r.at[i, m], (partner, d))

    def late_relay_in(i, m):
        at = gbuf.at[0, other_block_at(early + i), 1 - c, :, lanes(m)]
        return remote(at, at, f2s.at[i, m], f2r.at[i, m], (partner, d))

    def upper(w):
        @pl.when(top)
        def _():
            def one(o, carry):
                gbuf[1, o, c] = top_product(0, o)
                across(o).start()
                return carry

            lax.fori_loop(8 * w // SUBS, 8 * (w + 1) // SUBS, one, 0)

    def lower(r):
        o = block_at(r)

        @pl.when(r > 0)
        def _():
            for i in range(GIFTS):
                lift(i, o).wait_recv()

        obuf[o] = top_product(1, o)

        @pl.when(r < early)
        def _():
            down_hop(o).start()

        @pl.when(r >= early)
        def _():
            late_hop(r - early, 0).start()

    def hand_on(r):
        o = block_at(r)
        down_hop(o).wait_recv()
        relay(o).start()

    waves(1, 2, upper)

    @pl.when(top)
    def _():
        def one(o, carry):
            across_in(o).wait_recv()
            return carry

        lax.fori_loop(0, replicas, one, 0)
        ugb[1] = fdot(upb[1], whole(1)).astype(jnp.bfloat16)

    def middle(w):
        step, turn = w // SUBS, w % SUBS
        first = step == 0

        @pl.when(top & ((first & (turn < 5)) | ((step > 0) & ((turn == 2) | (turn == 4)))))
        def _():
            lower(jnp.where(first, turn, 3 + 2 * step + (turn - 2) // 2))

        few = jnp.where(step == 2, 3, 2)
        base = jnp.where(step == 1, 0, jnp.where(step == 2, 2, 2 * step - 1))

        @pl.when(second & (step > 0) & (turn >= 4) & (turn < 4 + few))
        def _():
            hand_on(base + turn - 4)

    waves(3, 5, middle)

    def final(w):
        @pl.when(top & ((w == 2) | (w == 4)))
        def _():
            lower(12 + w // 2)

        @pl.when(second & ((w == 4) | (w == 6)))
        def _():
            hand_on(7 + w // 2)

    waves(8, 1, final)

    @pl.when(top)
    def _():
        lower(replicas - 1)

        def one(m, carry):
            for i in range(LATE):
                late_hop(i, m).start()
            return carry

        lax.fori_loop(1, slots, one, 0)

    @pl.when(second)
    def _():
        hand_on(early - 1)

        def two(r, carry):
            relay_in(other_block_at(r)).wait_recv()
            return carry

        lax.fori_loop(0, early, two, 0)

    def terms(m):
        inputs = abuf[pl.ds(pl.multiple_of(m * tokens, tokens), tokens), :]
        down_term = fdot(ugb[mine, :, lanes(m)], inputs)
        up_term = fdot(dab[:, lanes(m)], part_of(mine, m), NT)
        tbuf[m, :rank, :] = down_term
        tbuf[m, rank:, :] = up_term
        square = jnp.sum(down_term * down_term + up_term * up_term, axis=0, keepdims=True)
        square = jnp.sum(square, axis=1, keepdims=True)
        sqbuf[pl.ds(m, 1), :] = jnp.broadcast_to(square, (1, LANES))

    def quad(ref, j, m, part, side):
        return ref.at[j, pl.ds(part * group, group), side, :, lanes(m)]

    def quad_product(j, m, part):
        blocks = pl.ds(part * group, group)
        weight = wbuf[j, blocks].reshape(group * half, features)
        adapter = dtb[j, blocks, c].reshape(group * half, rank)
        got = fdot(weight, part_of(j, m)) + fdot(adapter, ugb[j, :, lanes(m)])
        return got.astype(jnp.bfloat16).reshape(group, half, tokens)

    def quad_across(m, part, side):
        at = quad(gbuf, 1, m, part, side)
        return remote(at, at, es.at[m * QUADS + part], er.at[m * QUADS + part], (partner, d))

    def quad_down(m, part):
        src = obuf.at[pl.ds(part * group, group), :, lanes(m)]
        at = m * QUADS + part
        return remote(src, quad(gbuf, 0, m, part, c), ys.at[at], yr.at[at], (below, d))

    def quad_relay(m, part, side):
        at = quad(gbuf, 0, m, part, side)
        return remote(at, at, fs.at[m * QUADS + part], fr.at[m * QUADS + part], (partner, d))

    def each_quad(work):
        def one(part, carry):
            work(part)
            return carry

        lax.fori_loop(0, QUADS, one, 0)

    def odd_whole(m):
        ugb[0, :, lanes(m)] = fdot(upb[0], part_of(0, m)).astype(jnp.bfloat16)

        def odd(part):
            gbuf[1, pl.ds(part * group, group), c, :, lanes(m)] = quad_product(0, m, part)
            quad_across(m, part, c).start()

        each_quad(odd)

    def slot(m, carry):
        @pl.when(second)
        def _():
            for i in range(LATE):
                late_hop(i, m).wait_recv()
                late_relay(i, m).start()
            for i in range(LATE):
                late_relay_in(i, m).wait_recv()
            odd_whole(m)

        @pl.when(y < sections // 2 - 2)
        def _():
            def pass_on(part):
                quad_down(m, part).wait_recv()
                quad_relay(m, part, c).start()

            each_quad(pass_on)
            each_quad(lambda part: quad_relay(m, part, 1 - c).wait_recv())
            odd_whole(m)

        @pl.when(c == 1)
        def _():
            terms(m)

        @pl.when((c == 0) & (m > 0))
        def _():
            terms(m - 1)

        @pl.when((second | (y == 1)) & (m == 0))
        def _():
            def three(r, carry):
                for i in range(GIFTS):
                    lift(i, block_at(r)).wait_recv()
                return carry

            lax.fori_loop(1, replicas, three, 0)

        each_quad(lambda part: quad_across(m, part, 1 - c).wait_recv())
        ugb[1, :, lanes(m)] = fdot(upb[1], part_of(1, m)).astype(jnp.bfloat16)

        @pl.when(y > 0)
        def _():
            def even(part):
                obuf[pl.ds(part * group, group), :, lanes(m)] = quad_product(1, m, part)
                quad_down(m, part).start()

            each_quad(even)

        return carry

    def drain_rings():
        for copy in swaps(mine):
            copy.wait_send()
        for j in range(2):

            def one(w, carry):
                k, sub = 1 + w // SUBS, w % SUBS
                for way in range(2):

                    @pl.when(travels(j, sub) & ((k < last) | ours(way, sub)))
                    def _(way=way):
                        sending(j, way, k, sub).wait_send()

                return carry

            lax.fori_loop(0, last * SUBS, one, 0)

        @pl.when(given)
        def _():
            for i in range(GIFTS):
                gift(i).wait_send()

        for h in range(AIDS):

            @pl.when(h < aids)
            def _(h=h):
                for way in range(2):
                    for k in range(1, last + 1):
                        if k < last or way == 1 - h % 2:
                            aid_sending(h, way, k).wait_send()

                def one(r, carry):
                    lift(h, block_at(r)).wait_send()
                    return carry

                lax.fori_loop(1, replicas, one, 0)

    pl.when(y == 0)(drain_rings)

    @pl.when(y < sections // 2 - 1)
    def _():
        lax.fori_loop(0, slots, slot, 0)

        @pl.when(c == 0)
        def _():
            terms(slots - 1)

    @pl.when(top)
    def _():
        def one(m, carry):
            terms(m)
            return carry

        lax.fori_loop(0, slots, one, 0)

    def sq_hop(k):
        return remote(sqbuf, sqall.at[s], sqs.at[k], sqr.at[k], ((s + k) % sections, d))

    for k in range(1, sections):
        sq_hop(k).start()
    sqall[s] = sqbuf[...]
    pl.when(y > 0)(drain_rings)

    @pl.when(top)
    def _():
        def one(o, carry):
            across(o).wait_send()
            return carry

        lax.fori_loop(0, replicas, one, 0)

        def two(r, carry):
            down_hop(block_at(r)).wait_send()
            return carry

        lax.fori_loop(0, early, two, 0)

        def three(m, carry):
            for i in range(LATE):
                late_hop(i, m).wait_send()
            return carry

        lax.fori_loop(0, slots, three, 0)

    @pl.when(second)
    def _():
        def one(r, carry):
            relay(block_at(r)).wait_send()
            return carry

        lax.fori_loop(0, early, one, 0)

        def two(m, carry):
            for i in range(LATE):
                late_relay(i, m).wait_send()
            return carry

        lax.fori_loop(0, slots, two, 0)

    @pl.when(y < sections // 2 - 1)
    def _():
        def one(w, carry):
            m, part = w // QUADS, w % QUADS
            quad_across(m, part, c).wait_send()

            @pl.when(y > 0)
            def _():
                quad_down(m, part).wait_send()

            @pl.when(y < sections // 2 - 2)
            def _():
                quad_relay(m, part, c).wait_send()

            return carry

        lax.fori_loop(0, slots * QUADS, one, 0)

    for k in range(1, sections):
        sq_hop(k).wait_recv()
    norm = jnp.sqrt(jnp.sum(sqall[...], axis=0))
    lane = lax.broadcasted_iota(jnp.int32, (1, LANES), 1)
    named = jnp.zeros((1, LANES), jnp.float32)
    for m in range(slots):
        named = named + jnp.where(lane == ids_ref[0, m], norm[m : m + 1, :], 0.0)
    out_ref[2 * rank :, :LANES] = jnp.broadcast_to(named, (8, LANES))
    out_ref[2 * rank :, LANES:] = jnp.zeros((8, window - LANES), jnp.float32)
    factor = clip_scale / (norm + 0.01)
    total = factor[0:1, 0:1] * tbuf[0]
    for m in range(1, slots):
        total = total + factor[m : m + 1, 0:1] * tbuf[m]
    redsend[:, :features] = total.astype(jnp.bfloat16)

    def window_of(t):
        return pl.ds(pl.multiple_of(span * t // LANES * LANES, LANES), window)

    def red_hop(k):
        t = (d + k) % replicas
        return remote(redsend.at[:, window_of(t)], redin.at[d], rs.at[k], rr.at[k], (s, t))

    for k in range(1, replicas):
        red_hop(k).start()
    redin[d] = redsend[:, window_of(d)]
    for k in range(1, replicas):
        red_hop(k).wait_recv()
    reduced = jnp.sum(redin[...].astype(jnp.float32), axis=0)
    reduced = pltpu.roll(reduced, (window - span * d % LANES) % window, axis=1)
    out_ref[: 2 * rank] = reduced

    for k in range(1, sections):
        sq_hop(k).wait_send()
    for k in range(1, replicas):
        red_hop(k).wait_send()


def on_device(acts, cotangent, frozen, down_adapter, up_adapter, example_ids, lengths):
    sections = lax.axis_size("section")
    replicas = lax.axis_size("dp")
    layer_inputs = acts[0]
    slots = example_ids.shape[1]
    width, features = layer_inputs.shape
    tokens = width // slots
    rank = down_adapter.shape[1]
    clip_scale = math.sqrt(2.0 * rank * features) / math.sqrt(replicas * slots)
    span = features // replicas
    half = span // 2
    window = -(-(span + LANES - 1) // LANES) * LANES
    vmem = pl.BlockSpec(memory_space=pltpu.VMEM)
    smem = pl.BlockSpec(memory_space=pltpu.SMEM)
    hbm = pl.BlockSpec(memory_space=pl.ANY)
    dma = pltpu.SemaphoreType.DMA
    bf16, f32 = jnp.bfloat16, jnp.float32
    out = pl.pallas_call(
        functools.partial(kernel, sections, replicas, slots, clip_scale),
        out_shape=jax.ShapeDtypeStruct((2 * rank + 8, window), f32),
        in_specs=[hbm, hbm, hbm, vmem, vmem, smem, smem],
        out_specs=vmem,
        scratch_shapes=[
            pltpu.VMEM((2, replicas, half, features), bf16),
            pltpu.VMEM((2, replicas, 2, half, width), bf16),
            pltpu.VMEM((replicas, half, width), bf16),
            pltpu.VMEM((width, features), bf16),
            pltpu.VMEM((width, features), bf16),
            pltpu.VMEM((2, rank, features), bf16),
            pltpu.VMEM((2, rank, features), bf16),
            pltpu.VMEM((2, replicas, 2, half, rank), bf16),
            pltpu.VMEM((2, rank, width), bf16),
            pltpu.VMEM((rank, width), bf16),
            pltpu.VMEM((slots, 2 * rank, features), f32),
            pltpu.VMEM((8, LANES), f32),
            pltpu.VMEM((sections, 8, LANES), f32),
            pltpu.VMEM((2 * rank, features + LANES), bf16),
            pltpu.VMEM((replicas, 2 * rank, window), bf16),
            pltpu.VMEM((8, width), f32),
            dma((3,)), dma((3,)), dma((3,)),
            dma((2, 2, replicas // 2, SUBS)), dma((2, 2, replicas // 2, SUBS)),
            dma((replicas,)), dma((replicas,)),
            dma((replicas,)), dma((replicas,)),
            dma((replicas,)), dma((replicas,)),
            dma((sections,)), dma((sections,)),
            dma((replicas,)), dma((replicas,)),
            pltpu.VMEM((AIDS, replicas, half, features // SUBS), bf16),
            dma((GIFTS,)), dma((AIDS,)),
            dma((AIDS, 2, replicas // 2)), dma((AIDS, 2, replicas // 2)),
            dma((AIDS, replicas)), dma((GIFTS, replicas)),
            dma((LATE, slots)), dma((LATE, slots)), dma((LATE, slots)), dma((LATE, slots)),
        ],
        compiler_params=pltpu.CompilerParams(
            collective_id=0, has_side_effects=True, vmem_limit_bytes=62 * 1024 * 1024
        ),
    )(frozen[0], cotangent, layer_inputs, up_adapter[0], down_adapter[0], example_ids, lengths)
    return (out[None, :rank, :span], out[None, rank : 2 * rank, :span], out[2 * rank : 2 * rank + 1, :slots])


def solution(mesh):
    in_specs = (
        P("section", "dp", None),
        P("dp", None),
        P("section", "dp", None),
        P("section", None, None),
        P("section", None, None),
        P("dp", None),
        P("dp", None),
    )
    out_specs = (P("section", None, "dp"), P("section", None, "dp"), P("dp", None))
    return jax.shard_map(
        on_device, mesh=mesh, in_specs=in_specs, out_specs=out_specs, check_vma=False
    )
```
